16 devices in a mesh: dp: 2 (over y, z), tp: 8 (over x, core).
Axes of the slice: x: 4, y: 2, z: 1, core: 2. Of those that a mesh axis runs over, the one named last changes fastest.
The devices are a block of a 4x4x8 slice.
Arguments:
- x_in: bfloat16 [4224, 3072], P(('dp', 'tp')), parts along dimension 0
- req_ids: int32 [4224], P('dp'), parts along dimension 0
- positions: int32 [4224], P('dp'), parts along dimension 0
- block_table: int32 [130, 256], P('dp'), parts along dimension 0
- ctx_len: int32 [130], P('dp'), parts along dimension 0
- k_pages: bfloat16 [8704, 16, 8, 128], P('dp', None, 'tp'), parts along dimension 0
- v_pages: bfloat16 [8704, 16, 8, 128], P('dp', None, 'tp'), parts along dimension 0
- w_q: bfloat16 [3072, 3072], P(None, 'tp')
- w_k: bfloat16 [3072, 1024], P(None, 'tp')
- w_v: bfloat16 [3072, 1024], P(None, 'tp')
- w_o: bfloat16 [3072, 3072], P('tp')
- w_gate: bfloat16 [3072, 8192], P(None, 'tp')
- w_up: bfloat16 [3072, 8192], P(None, 'tp')
- w_down: bfloat16 [8192, 3072], P('tp')
- g_attn: bfloat16 [3072], replicated
- g_mlp: bfloat16 [3072], replicated
Outputs:
- output 1: bfloat16 [4224, 3072], P(('dp', 'tp')), parts along dimension 0
- output 2: bfloat16 [8704, 16, 8, 128], P('dp', None, 'tp'), parts along dimension 0
- output 3: bfloat16 [8704, 16, 8, 128], P('dp', None, 'tp'), parts along dimension 0
There are 2 independent parts. The reference program is written for one: setup_inputs(seed, part) draws one part's arguments, and reference() takes and returns one part's arrays. A program takes and returns all parts, laid end to end along the dimension named above; an argument that names none is the same for every part.
All inputs are finite; a program needn't handle non-finite values.
Results may differ from the reference program's by a relative error of at most 0.0160456.
Values are sent between devices in bfloat16 or wider.
A program may use at most 768 MiB of HBM per device.

```python
import jax
import jax.numpy as jnp
from jax import lax

D_MODEL = 3072
HEADS = 24
KV_HEADS = 8
HEAD = 128
FF = 8192
CHUNK = 2048
DECODE = 64
PREFIX = 2048
DEC_CTX = 1024
PAGE = 16
QUERY_BLOCK = 128
DECODE_BLOCK = 8

EPS = 1e-5
THETA = 500000.0
K_SCALE = 2.5
V_SCALE = 1.5
TOKENS = CHUNK + DECODE
REQS = DECODE + 1
CHUNK_PAGES = (PREFIX + CHUNK) // PAGE
DEC_PAGES = DEC_CTX // PAGE
TABLE_WIDTH = max(CHUNK_PAGES, DEC_PAGES)
POOL = CHUNK_PAGES + DECODE * DEC_PAGES
GROUP_REP = HEADS // KV_HEADS


def draw_layout(layout_key):
    subkeys = jax.random.split(layout_key, 5)
    req_order = jax.random.permutation(subkeys[0], REQS).astype(jnp.int32)
    dec_len = jax.random.randint(subkeys[1], (DECODE,), DEC_CTX // 4, DEC_CTX + 1, dtype=jnp.int32)
    longest = jax.random.randint(subkeys[2], (), 0, DECODE, dtype=jnp.int32)
    dec_len = jnp.where(jnp.arange(DECODE) == longest, DEC_CTX, dec_len).astype(jnp.int32)
    slot_len = jnp.concatenate([jnp.full((1,), PREFIX + CHUNK, jnp.int32), dec_len])
    inverse = jnp.argsort(req_order)
    ctx_len = slot_len[inverse]
    req_ids = jnp.concatenate([jnp.full((CHUNK,), req_order[0], jnp.int32), req_order[1:]])
    positions = jnp.concatenate([PREFIX + jnp.arange(CHUNK, dtype=jnp.int32), dec_len - 1])
    page_order = jax.random.permutation(subkeys[3], POOL).astype(jnp.int32)
    slot_table = jax.random.randint(subkeys[4], (REQS, TABLE_WIDTH), 0, POOL, dtype=jnp.int32)
    slot_table = slot_table.at[0, :CHUNK_PAGES].set(page_order[:CHUNK_PAGES])
    slot_table = slot_table.at[1:, :DEC_PAGES].set(page_order[CHUNK_PAGES:].reshape(DECODE, DEC_PAGES))
    block_table = slot_table[inverse]
    return req_ids, positions, block_table, ctx_len


def draw_dense(weight_key, fan_in, fan_out, gain):
    return (gain * fan_in ** -0.5 * jax.random.normal(weight_key, (fan_in, fan_out), jnp.float32)).astype(jnp.bfloat16)


def setup_inputs(seed: int = 0, part: int = 0) -> dict:
    base_key = jax.random.key(seed)
    part_keys = jax.random.split(jax.random.fold_in(base_key, part), 4)
    weight_keys = jax.random.split(base_key, 9)
    req_ids, positions, block_table, ctx_len = draw_layout(part_keys[0])
    cache_shape = (POOL, PAGE, KV_HEADS, HEAD)
    return {
        'x_in': jax.random.normal(part_keys[1], (TOKENS, D_MODEL), jnp.float32).astype(jnp.bfloat16),
        'req_ids': req_ids,
        'positions': positions,
        'block_table': block_table,
        'ctx_len': ctx_len,
        'k_pages': (K_SCALE * jax.random.normal(part_keys[2], cache_shape, jnp.float32)).astype(jnp.bfloat16),
        'v_pages': (V_SCALE * jax.random.normal(part_keys[3], cache_shape, jnp.float32)).astype(jnp.bfloat16),
        'w_q': draw_dense(weight_keys[0], D_MODEL, HEADS * HEAD, 1.0),
        'w_k': draw_dense(weight_keys[1], D_MODEL, KV_HEADS * HEAD, K_SCALE),
        'w_v': draw_dense(weight_keys[2], D_MODEL, KV_HEADS * HEAD, V_SCALE),
        'w_o': draw_dense(weight_keys[3], HEADS * HEAD, D_MODEL, 1.0),
        'w_gate': draw_dense(weight_keys[4], D_MODEL, FF, 1.0),
        'w_up': draw_dense(weight_keys[5], D_MODEL, FF, 1.0),
        'w_down': draw_dense(weight_keys[6], FF, D_MODEL, 1.0),
        'g_attn': jax.random.uniform(weight_keys[7], (D_MODEL,), jnp.float32, 0.5, 1.5).astype(jnp.bfloat16),
        'g_mlp': jax.random.uniform(weight_keys[8], (D_MODEL,), jnp.float32, 0.5, 1.5).astype(jnp.bfloat16),
    }


def rms_norm(rows, gain):
    rows32 = rows.astype(jnp.float32)
    inv_rms = lax.rsqrt(jnp.mean(rows32 * rows32, axis=-1, keepdims=True) + EPS)
    return (rows32 * inv_rms * gain.astype(jnp.float32)).astype(jnp.bfloat16)


def rotary(vals, positions):
    half_dim = vals.shape[-1] // 2
    inv_freq = THETA ** (-jnp.arange(half_dim, dtype=jnp.float32) * 2.0 / vals.shape[-1])
    angles = positions.astype(jnp.float32)[:, None] * inv_freq[None, :]
    cosine = jnp.cos(angles)[:, None, :]
    sine_val = jnp.sin(angles)[:, None, :]
    vals32 = vals.astype(jnp.float32)
    first_half = vals32[..., :half_dim]
    second_half = vals32[..., half_dim:]
    return jnp.concatenate([first_half * cosine - second_half * sine_val, second_half * cosine + first_half * sine_val], axis=-1).astype(jnp.bfloat16)


def softmax_mix(scores, key_mask, form, values):
    scores = jnp.where(key_mask, scores, -1e30)
    row_max = jnp.max(scores, axis=-1, keepdims=True)
    weights = jnp.exp(scores - row_max)
    weight_sum = jnp.sum(weights, axis=-1, keepdims=True)
    mixed_out = jnp.einsum(form, weights.astype(jnp.bfloat16).astype(jnp.float32), values)
    return (mixed_out / weight_sum).astype(jnp.bfloat16)


def reference(x_in, req_ids, positions, block_table, ctx_len, k_pages, v_pages, w_q, w_k, w_v, w_o, w_gate, w_up, w_down, g_attn, g_mlp):
    hidden = rms_norm(x_in, g_attn)
    q_rows = jnp.dot(hidden, w_q, preferred_element_type=jnp.float32).astype(jnp.bfloat16).reshape(TOKENS, HEADS, HEAD)
    k_rows = jnp.dot(hidden, w_k, preferred_element_type=jnp.float32).astype(jnp.bfloat16).reshape(TOKENS, KV_HEADS, HEAD)
    v_rows = jnp.dot(hidden, w_v, preferred_element_type=jnp.float32).astype(jnp.bfloat16).reshape(TOKENS, KV_HEADS, HEAD)
    q_rows = rotary(q_rows, positions)
    k_rows = rotary(k_rows, positions)
    page_ids = block_table[req_ids, positions // PAGE]
    slot_ids = positions % PAGE
    k_cache = k_pages.at[page_ids, slot_ids].set(k_rows)
    v_cache = v_pages.at[page_ids, slot_ids].set(v_rows)
    last_key = jnp.minimum(positions, ctx_len[req_ids] - 1)
    key_pos = jnp.arange(TABLE_WIDTH * PAGE)
    attn_scale = HEAD ** -0.5
    chunk_row = block_table[req_ids[0]]
    chunk_keys = k_cache[chunk_row].reshape(TABLE_WIDTH * PAGE, KV_HEADS, HEAD).astype(jnp.float32)
    chunk_vals = v_cache[chunk_row].reshape(TABLE_WIDTH * PAGE, KV_HEADS, HEAD).astype(jnp.float32)

    def chunk_block(block_args):
        q_blk, last_blk = block_args
        scores = jnp.einsum('bgrd,tgd->bgrt', q_blk.astype(jnp.float32), chunk_keys) * attn_scale
        key_mask = (key_pos[None, :] <= last_blk[:, None])[:, None, None, :]
        return softmax_mix(scores, key_mask, 'bgrt,tgd->bgrd', chunk_vals)

    chunk_out = lax.map(chunk_block, (q_rows[:CHUNK].reshape(CHUNK // QUERY_BLOCK, QUERY_BLOCK, KV_HEADS, GROUP_REP, HEAD), last_key[:CHUNK].reshape(CHUNK // QUERY_BLOCK, QUERY_BLOCK)))

    def decode_block(block_args):
        q_blk, req_blk, last_blk = block_args
        rows_blk = block_table[req_blk]
        keys_blk = k_cache[rows_blk].reshape(DECODE_BLOCK, TABLE_WIDTH * PAGE, KV_HEADS, HEAD).astype(jnp.float32)
        vals_blk = v_cache[rows_blk].reshape(DECODE_BLOCK, TABLE_WIDTH * PAGE, KV_HEADS, HEAD).astype(jnp.float32)
        scores = jnp.einsum('bgrd,btgd->bgrt', q_blk.astype(jnp.float32), keys_blk) * attn_scale
        key_mask = (key_pos[None, :] <= last_blk[:, None])[:, None, None, :]
        return softmax_mix(scores, key_mask, 'bgrt,btgd->bgrd', vals_blk)

    dec_blocks = DECODE // DECODE_BLOCK
    dec_out = lax.map(decode_block, (q_rows[CHUNK:].reshape(dec_blocks, DECODE_BLOCK, KV_HEADS, GROUP_REP, HEAD), req_ids[CHUNK:].reshape(dec_blocks, DECODE_BLOCK), last_key[CHUNK:].reshape(dec_blocks, DECODE_BLOCK)))
    attn_rows = jnp.concatenate([chunk_out.reshape(CHUNK, HEADS * HEAD), dec_out.reshape(DECODE, HEADS * HEAD)], axis=0)
    attn_proj = jnp.dot(attn_rows, w_o, preferred_element_type=jnp.float32)
    mid_rows = (x_in.astype(jnp.float32) + attn_proj).astype(jnp.bfloat16)
    hidden_mlp = rms_norm(mid_rows, g_mlp)
    gate_proj = jnp.dot(hidden_mlp, w_gate, preferred_element_type=jnp.float32)
    up_proj = jnp.dot(hidden_mlp, w_up, preferred_element_type=jnp.float32)
    act_rows = (jax.nn.silu(gate_proj) * up_proj).astype(jnp.bfloat16)
    down_proj = jnp.dot(act_rows, w_down, preferred_element_type=jnp.float32)
    x_out = (mid_rows.astype(jnp.float32) + down_proj).astype(jnp.bfloat16)
    return x_out, k_cache, v_cache
```

```python
import functools

import jax
import jax.numpy as jnp
from jax import lax
from jax.experimental import pallas as pl
from jax.experimental.pallas import tpu as pltpu
from jax.sharding import PartitionSpec as P

EPS = 1e-5
THETA = 500000.0
LOG2E = 1.4426950408889634
ANY = pl.BlockSpec(memory_space=pl.ANY)
SMEM = pl.BlockSpec(memory_space=pltpu.SMEM)
VMEM = pl.BlockSpec(memory_space=pltpu.VMEM)


def rms_norm(rows, gain):
    rows32 = rows.astype(jnp.float32)
    inv_rms = lax.rsqrt(jnp.mean(rows32 * rows32, axis=-1, keepdims=True) + EPS)
    return (rows32 * inv_rms * gain.astype(jnp.float32)).astype(jnp.bfloat16)


def cost(flops, nbytes):
    return pl.CostEstimate(flops=int(flops), bytes_accessed=int(nbytes), transcendentals=0)


def stage_kernel(dec_pages, pre_pages, parts, table, reqs, kp, vp, ko, vo, kd, vd, kc, vc,
                 kbuf, vbuf, stage, in_sem, out_sem, stage_sem):
    pool, page, _ = kbuf.shape
    step = pool // parts
    n_dec = kd.shape[0]
    chunk_len = reqs.shape[0] - n_dec
    span = dec_pages * page

    def copy_in(c, src, buf, i):
        return pltpu.make_async_copy(src.at[pl.ds(i * step, step)], buf.at[pl.ds(i * step, step)], in_sem.at[c, i])

    def copy_out(c, buf, dst, i):
        return pltpu.make_async_copy(buf.at[pl.ds(i * step, step)], dst.at[pl.ds(i * step, step)], out_sem.at[c, i])

    pairs = ((kp, kbuf, ko, kd, kc), (vp, vbuf, vo, vd, vc))
    for c, (src, buf, _, _, _) in enumerate(pairs):
        for i in range(parts):
            copy_in(c, src, buf, i).start()

    def put(slot, dst):
        return pltpu.make_async_copy(stage.at[slot], dst, stage_sem.at[slot])

    for c, (src, buf, dst, dec, pre) in enumerate(pairs):
        for i in range(parts):
            copy_in(c, src, buf, i).wait()
            copy_out(c, buf, dst, i).start()

        def gather(req, first, slot, buf=buf):
            for j in range(dec_pages):
                stage[slot, pl.ds(j * page, page), :] = buf[table[req, first + j]]

        for g in range(pre_pages // dec_pages):
            slot = g % 2
            if g >= 2 or c > 0:
                put(slot, pre.at[pl.ds(0, span)]).wait()
            gather(reqs[0], g * dec_pages, slot)
            put(slot, pre.at[pl.ds(g * span, span)]).start()

        def body(i, carry, dec=dec):
            slot = lax.rem(i, 2)
            put(slot, dec.at[0]).wait()
            gather(reqs[chunk_len + i], 0, slot)
            put(slot, dec.at[i]).start()
            return carry

        lax.fori_loop(0, n_dec, body, 0)
    for slot in range(2):
        put(slot, vd.at[0]).wait()
    for c, (_, buf, dst, _, _) in enumerate(pairs):
        for i in range(parts):
            copy_out(c, buf, dst, i).wait()


def stage_cache(table, reqs, kp, vp, n_dec, dec_pages, pre_pages):
    pool, page, head = kp.shape
    parts = 4
    bf = jnp.bfloat16
    dec = jax.ShapeDtypeStruct((n_dec, dec_pages * page, head), bf)
    pre = jax.ShapeDtypeStruct((pre_pages * page, head), bf)
    full = jax.ShapeDtypeStruct(kp.shape, bf)
    return pl.pallas_call(
        functools.partial(stage_kernel, dec_pages, pre_pages, parts),
        out_shape=[full, full, dec, dec, pre, pre],
        in_specs=[SMEM, SMEM, ANY, ANY],
        out_specs=[ANY] * 6,
        scratch_shapes=[
            pltpu.VMEM((pool, page, head), bf),
            pltpu.VMEM((pool, page, head), bf),
            pltpu.VMEM((2, dec_pages * page, head), bf),
            pltpu.SemaphoreType.DMA((2, parts)),
            pltpu.SemaphoreType.DMA((2, parts)),
            pltpu.SemaphoreType.DMA((2,)),
        ],
        compiler_params=pltpu.CompilerParams(vmem_limit_bytes=40 * 2**20),
        cost_estimate=cost(4e10, 1e8),
        name="stage_cache",
    )(table, reqs, kp, vp)


def qkv_kernel(head, n_q, h, w, cs, sn, q_out, k_out, v_out):
    cos, sin = cs[...], sn[...]
    x = jnp.dot(h[...], w[...], preferred_element_type=jnp.float32).astype(jnp.bfloat16)
    for n in range(n_q + 1):
        part = x[:, n * head:(n + 1) * head].astype(jnp.float32)
        val = (part * cos + pltpu.roll(part, head // 2, 1) * sin).astype(jnp.bfloat16)
        if n < n_q:
            q_out[n] = val
        else:
            k_out[...] = val
    v_out[...] = x[:, (n_q + 1) * head:]


def qkv(hidden, w, cos, sin, head):
    tokens, d = hidden.shape
    cols = w.shape[1]
    n_q = cols // head - 2
    blk = tokens // 4
    bf = jnp.bfloat16
    row = lambda c: pl.BlockSpec((blk, c), lambda i: (i, 0))
    return pl.pallas_call(
        functools.partial(qkv_kernel, head, n_q),
        grid=(tokens // blk,),
        out_shape=[
            jax.ShapeDtypeStruct((n_q, tokens, head), bf),
            jax.ShapeDtypeStruct((tokens, head), bf),
            jax.ShapeDtypeStruct((tokens, head), bf),
        ],
        in_specs=[row(d), pl.BlockSpec((d, cols), lambda i: (0, 0)), row(head), row(head)],
        out_specs=[pl.BlockSpec((n_q, blk, head), lambda i: (0, i, 0)), row(head), row(head)],
        compiler_params=pltpu.CompilerParams(vmem_limit_bytes=40 * 2**20),
        cost_estimate=cost(2 * tokens * d * cols, 2 * tokens * d),
        name="qkv",
    )(hidden, w, cos, sin)


def chunk_kernel(bq, bk, scale, q, kc, vc, kn, vn, out, acc, m_ref, l_ref):
    b = pl.program_id(0)
    n_q, _, head = q.shape
    rows = n_q * bq
    qq = q[...].reshape(rows, head)
    m_ref[...] = jnp.full_like(m_ref, -jnp.inf)
    l_ref[...] = jnp.zeros_like(l_ref)
    acc[...] = jnp.zeros_like(acc)

    def attend(keys, vals, masked):
        s = lax.dot_general(qq, keys, (((1,), (1,)), ((), ())), preferred_element_type=jnp.float32)
        if masked:
            i = lax.rem(lax.broadcasted_iota(jnp.int32, s.shape, 0), bq)
            j = lax.broadcasted_iota(jnp.int32, s.shape, 1)
            s = jnp.where(j <= i, s, -1e30)
        m_old = m_ref[...]
        m_new = jnp.maximum(m_old, jnp.max(s, axis=-1, keepdims=True))
        alpha = jnp.exp2((m_old - m_new) * scale)
        p = jnp.exp2((s - m_new[:, :1]) * scale)
        l_ref[...] = l_ref[...] * alpha + jnp.sum(p, axis=-1, keepdims=True)
        acc[...] = acc[...] * alpha + jnp.dot(p.astype(jnp.bfloat16), vals, preferred_element_type=jnp.float32)
        m_ref[...] = m_new

    def pre(t, carry):
        sl = pl.ds(pl.multiple_of(t * bk, bk), bk)
        attend(kc[sl, :], vc[sl, :], False)
        return carry

    lax.fori_loop(0, kc.shape[0] // bk, pre, 0)

    def new(t, carry):
        sl = pl.ds(pl.multiple_of(t * bq, bq), bq)
        attend(kn[sl, :], vn[sl, :], False)
        return carry

    lax.fori_loop(0, b, new, 0)
    sl = pl.ds(pl.multiple_of(b * bq, bq), bq)
    attend(kn[sl, :], vn[sl, :], True)
    o = (acc[...] / l_ref[...]).astype(jnp.bfloat16).reshape(n_q, bq, head)
    for n in range(n_q):
        out[:, n * head:(n + 1) * head] = o[n]


def chunk_attention(q, kc, vc, kn, vn, chunk_len):
    n_q, _, head = q.shape
    bq, bk = 256, 512
    scale = head ** -0.5 * LOG2E
    whole = lambda a: pl.BlockSpec((a.shape[0], head), lambda i: (0, 0))
    new = pl.BlockSpec((chunk_len, head), lambda i: (0, 0))
    pre_len = kc.shape[0]
    return pl.pallas_call(
        functools.partial(chunk_kernel, bq, bk, scale),
        grid=(chunk_len // bq,),
        out_shape=jax.ShapeDtypeStruct((chunk_len, n_q * head), jnp.bfloat16),
        in_specs=[pl.BlockSpec((n_q, bq, head), lambda i: (0, i, 0)), whole(kc), whole(vc), new, new],
        out_specs=pl.BlockSpec((bq, n_q * head), lambda i: (i, 0)),
        scratch_shapes=[pltpu.VMEM((n_q * bq, head), jnp.float32)] * 3,
        compiler_params=pltpu.CompilerParams(vmem_limit_bytes=32 * 2**20),
        cost_estimate=cost(4 * chunk_len * (pre_len + chunk_len // 2) * head * n_q, 4 * pre_len * head * 2),
        name="chunk_attention",
    )(q, kc, vc, kn, vn)


def decode_kernel(group, scale, n_q, chunk_len, pos, q, kd, vd, kn, vn, out):
    g = pl.program_id(0)
    _, pad, head = q.shape
    span = kd.shape[1]
    col = lax.broadcasted_iota(jnp.int32, (pad, span), 1)
    for r in range(group):
        p0 = pos[chunk_len + g * group + r]
        qr = q[r]
        self_k, self_v = kn[r].astype(jnp.float32), vn[r].astype(jnp.float32)
        s = lax.dot_general(qr, kd[r], (((1,), (1,)), ((), ())), preferred_element_type=jnp.float32)
        s_self = jnp.sum(qr.astype(jnp.float32) * self_k, axis=-1, keepdims=True)
        s = jnp.where(col < p0, s, -1e30)
        m = jnp.maximum(jnp.max(s, axis=-1, keepdims=True), s_self)
        p = jnp.exp2((s - m) * scale)
        p_self = jnp.exp2((s_self - m) * scale)
        l = jnp.sum(p, axis=-1, keepdims=True) + p_self
        o = jnp.dot(p.astype(jnp.bfloat16), vd[r], preferred_element_type=jnp.float32)
        o = o + p_self.astype(jnp.bfloat16).astype(jnp.float32) * self_v
        out[r] = (o / l).astype(jnp.bfloat16)


def decode_attention(pos, q, kd, vd, kn, vn, n_q):
    n_dec, pad, head = q.shape
    span = kd.shape[1]
    group = 8
    scale = head ** -0.5 * LOG2E
    blk = lambda n: pl.BlockSpec((group, n, head), lambda i: (i, 0, 0))
    return pl.pallas_call(
        functools.partial(decode_kernel, group, scale, n_q, pos.shape[0] - n_dec),
        grid=(n_dec // group,),
        out_shape=jax.ShapeDtypeStruct((n_dec, pad, head), jnp.bfloat16),
        in_specs=[SMEM, blk(pad), blk(span), blk(span), blk(1), blk(1)],
        out_specs=blk(pad),
        compiler_params=pltpu.CompilerParams(vmem_limit_bytes=32 * 2**20),
        cost_estimate=cost(2e10, 4 * n_dec * span * head),
        name="decode_attention",
    )(pos, q, kd, vd, kn, vn)


def update_kernel(pre_pages, table, reqs, pos, kn, vn, ki, vi, ko, vo, pages, sem, sem2):
    page = ki.shape[1]
    n_dec = pages.shape[1]
    chunk_len = reqs.shape[0] - n_dec
    chunk_pages = chunk_len // page
    req0 = reqs[0]
    pairs = ((kn, ki, ko), (vn, vi, vo))

    def dec_page(i):
        return table[reqs[chunk_len + i], pos[chunk_len + i] // page]

    for c, (new, old, out) in enumerate(pairs):

        def start(i, carry, c=c, old=old):
            pltpu.make_async_copy(old.at[dec_page(i)], pages.at[c, i], sem.at[c]).start()
            return carry

        lax.fori_loop(0, n_dec, start, 0)

        def put(i, carry, c=c, new=new, out=out):
            rows = pl.ds(pl.multiple_of(i * page, page), page)
            pltpu.make_async_copy(new.at[rows, :], out.at[table[req0, pre_pages + i]], sem2.at[c]).start()
            return carry

        lax.fori_loop(0, chunk_pages, put, 0, unroll=8)
    for c, (new, old, out) in enumerate(pairs):
        pltpu.make_async_copy(old.at[pl.ds(0, n_dec)], pages.at[c], sem.at[c]).wait()
        for i in range(n_dec):
            slot = lax.rem(pos[chunk_len + i], page)
            hit = lax.broadcasted_iota(jnp.int32, pages.shape[2:], 0) == slot
            row = jnp.broadcast_to(new[pl.ds(chunk_len + i, 1), :].astype(jnp.float32), pages.shape[2:])
            pages[c, i] = jnp.where(hit, row, pages[c, i].astype(jnp.float32)).astype(jnp.bfloat16)
    for c, (new, old, out) in enumerate(pairs):

        def back(i, carry, c=c, out=out):
            pltpu.make_async_copy(pages.at[c, i], out.at[dec_page(i)], sem.at[c]).start()
            return carry

        lax.fori_loop(0, n_dec, back, 0)
    for c, (new, old, out) in enumerate(pairs):
        pltpu.make_async_copy(pages.at[c], out.at[pl.ds(0, n_dec)], sem.at[c]).wait()
        pltpu.make_async_copy(new.at[pl.ds(0, chunk_len), :], new.at[pl.ds(0, chunk_len), :], sem2.at[c]).wait()


def update_cache(table, reqs, pos, kn, vn, k_all, v_all, n_dec, pre_pages):
    page, head = k_all.shape[1:]
    full = jax.ShapeDtypeStruct(k_all.shape, jnp.bfloat16)
    return pl.pallas_call(
        functools.partial(update_kernel, pre_pages),
        out_shape=[full, full],
        in_specs=[SMEM, SMEM, SMEM, VMEM, VMEM, ANY, ANY],
        out_specs=[ANY, ANY],
        input_output_aliases={5: 0, 6: 1},
        scratch_shapes=[
            pltpu.VMEM((2, n_dec, page, head), jnp.bfloat16),
            pltpu.SemaphoreType.DMA((2,)),
            pltpu.SemaphoreType.DMA((2,)),
        ],
        compiler_params=pltpu.CompilerParams(vmem_limit_bytes=16 * 2**20),
        cost_estimate=cost(4e9, 1e6),
        name="update_cache",
    )(table, reqs, pos, kn, vn, k_all, v_all)


def rope_tables(positions, head):
    half = head // 2
    inv_freq = THETA ** (-jnp.arange(half, dtype=jnp.float32) * 2.0 / head)
    angles = positions.astype(jnp.float32)[:, None] * inv_freq[None, :]
    cos, sin = jnp.cos(angles), jnp.sin(angles)
    return jnp.concatenate([cos, cos], axis=1), jnp.concatenate([-sin, sin], axis=1)


def ring_places(tp):
    chips = tp // 2
    me = lax.axis_index('tp')
    chip, core = me // 2, lax.rem(me, 2)
    sign = 1 - 2 * core
    peer = 2 * chip + 1 - core

    def chip_at(offset):
        return lax.rem(chip + sign * offset + 2 * chips, chips)

    return chip, core, peer, chip_at


def greet(*others):
    barrier = pltpu.get_barrier_semaphore()
    for other in others:
        pl.semaphore_signal(barrier, inc=1, device_id={'tp': other}, device_id_type=pl.DeviceIdType.MESH)
    pl.semaphore_wait(barrier, len(others))


def remote(src, dst, send, recv, to):
    return pltpu.make_async_remote_copy(src_ref=src, dst_ref=dst, send_sem=send, recv_sem=recv, device_id={'tp': to}, device_id_type=pl.DeviceIdType.MESH)


def proj_kernel(tp, parts, attn, w_o, x, g, mid_out, hid_out,
                psend, precv, ssend, rrecv, total, ps_sem, pr_sem, ss_sem, rr_sem):
    chips = tp // 2
    chip, core, peer, chip_at = ring_places(tp)
    nxt = 2 * chip_at(1) + core
    prv = 2 * chip_at(-1) + core
    wide = total.shape[2]
    greet(peer, nxt, prv)

    def to_peer(s, q):
        return remote(psend.at[s, q], precv.at[s, q], ps_sem.at[s, q], pr_sem.at[s, q], peer)

    def to_next(s, q):
        return remote(ssend.at[s, q], rrecv.at[s, q], ss_sem.at[s, q], rr_sem.at[s, q], nxt)

    def product(block, q):
        cols = pl.ds(pl.multiple_of(q * wide, wide), wide)
        return jnp.dot(attn[block], w_o[:, cols], preferred_element_type=jnp.float32)

    for s in range(chips):
        theirs = 2 * chip_at(s + 1) + 1 - core
        mine = 2 * chip_at(-(s + 1)) + core

        def give(q, carry, s=s, theirs=theirs):
            psend[s, q] = product(theirs, q).astype(jnp.bfloat16)
            to_peer(s, q).start()
            return carry

        lax.fori_loop(0, parts, give, 0)

        def take(q, carry, s=s, mine=mine):
            own = product(mine, q)
            to_peer(s, q).wait_recv()
            own = own + precv[s, q].astype(jnp.float32)
            if s > 0:
                to_next(s - 1, q).wait_recv()
                own = own + rrecv[s - 1, q].astype(jnp.float32)
            if s < chips - 1:
                ssend[s, q] = own.astype(jnp.bfloat16)
                to_next(s, q).start()
            else:
                total[q] = own
            return carry

        lax.fori_loop(0, parts, take, 0)

    for q in range(parts):
        cols = slice(q * wide, (q + 1) * wide)
        mid = (x[:, cols].astype(jnp.float32) + total[q].astype(jnp.bfloat16).astype(jnp.float32)).astype(jnp.bfloat16)
        mid_out[:, cols] = mid
        total[q] = mid.astype(jnp.float32)
    square = sum(jnp.sum(total[q] * total[q], axis=-1, keepdims=True) for q in range(parts))
    inv_rms = lax.rsqrt(square / (parts * wide) + EPS)
    for q in range(parts):
        cols = slice(q * wide, (q + 1) * wide)
        hid_out[:, cols] = (total[q] * inv_rms * g[:, cols].astype(jnp.float32)).astype(jnp.bfloat16)
    for s in range(chips):
        for q in range(parts):
            to_peer(s, q).wait_send()
            if s < chips - 1:
                to_next(s, q).wait_send()


def project(tp, attn, w_o, x, g):
    rows, d = x.shape
    parts = 3
    wide = d // parts
    chips = tp // 2
    bf = jnp.bfloat16
    dma = pltpu.SemaphoreType.DMA
    block = lambda n: pltpu.VMEM((n, parts, rows, wide), bf)
    out = jax.ShapeDtypeStruct((rows, d), bf)
    return pl.pallas_call(
        functools.partial(proj_kernel, tp, parts),
        out_shape=[out, out],
        in_specs=[VMEM] * 4,
        out_specs=[VMEM] * 2,
        scratch_shapes=[
            block(chips), block(chips), block(chips - 1), block(chips - 1),
            pltpu.VMEM((parts, rows, wide), jnp.float32),
            dma((chips, parts)), dma((chips, parts)), dma((chips - 1, parts)), dma((chips - 1, parts)),
        ],
        compiler_params=pltpu.CompilerParams(collective_id=1, has_side_effects=True, vmem_limit_bytes=60 * 2**20),
        cost_estimate=cost(6e10, 1e7),
        name="project",
    )(attn, w_o, x, g.reshape(1, d))


def mlp_kernel(tp, parts, hid, mid, w_gate, w_up, w_down, out,
               hbuf, gbuf, ubuf, dbuf, xbuf, act, acc, last, psend, precv, ssend, rrecv,
               in_sem, ag_s, ag_r, pg_s, pg_r, ps_sem, pr_sem, ss_sem, rr_sem):
    chips = tp // 2
    chip, core, peer, chip_at = ring_places(tp)
    nxt = 2 * chip_at(1) + core
    prv = 2 * chip_at(-1) + core
    _, rows, wide = acc.shape
    ff = gbuf.shape[1]
    tile = 256
    cut = 144
    halves = ((0, cut), (cut, rows - cut))
    loads = [pltpu.make_async_copy(a, b, in_sem.at[i]) for i, (a, b) in enumerate(
        ((hid, hbuf.at[0]), (w_gate, gbuf), (w_up, ubuf), (w_down, dbuf), (mid, xbuf)))]
    for load in loads:
        load.start()
    greet(peer, nxt, prv)

    def gather(j, i):
        first, n = halves[i]
        cut_rows = pl.ds(first, n)
        return remote(hbuf.at[j, cut_rows], hbuf.at[j + 1, cut_rows], ag_s.at[j, i], ag_r.at[j, i], nxt)

    def share(j):
        return remote(hbuf.at[j], hbuf.at[chips + j], pg_s.at[j], pg_r.at[j], peer)

    def to_peer(s, q):
        return remote(psend.at[s % 2, q], precv.at[s, q], ps_sem.at[s, q], pr_sem.at[s, q], peer)

    def to_next(s, q):
        return remote(ssend.at[s % 2, q], rrecv.at[s, q], ss_sem.at[s, q], rr_sem.at[s, q], nxt)

    def hidden_act(j):
        def body(t, carry):
            cols = pl.ds(pl.multiple_of(t * tile, tile), tile)
            gate = jnp.dot(hbuf[j], gbuf[:, cols], preferred_element_type=jnp.float32)
            up = jnp.dot(hbuf[j], ubuf[:, cols], preferred_element_type=jnp.float32)
            act[:, cols] = (gate * jax.nn.sigmoid(gate) * up).astype(jnp.bfloat16)
            return carry

        lax.fori_loop(0, ff // tile, body, 0)

    def down(q):
        cols = pl.ds(pl.multiple_of(q * wide, wide), wide)
        return jnp.dot(act[...], dbuf[:, cols], preferred_element_type=jnp.float32)

    def keep(j, dst):
        hidden_act(j)

        def body(q, carry):
            dst[q] = down(q)
            return carry

        lax.fori_loop(0, parts, body, 0)

    def give(j, s, before):
        hidden_act(j)

        def body(q, carry):
            if before is not None:
                to_peer(before, q).wait_send()
            psend[s % 2, q] = down(q).astype(jnp.bfloat16)
            to_peer(s, q).start()
            return carry

        lax.fori_loop(0, parts, body, 0)

    loads[0].wait()
    for i in range(2):
        gather(0, i).start()
    share(0).start()
    for load in loads[1:4]:
        load.wait()
    keep(0, last)
    share(0).wait_recv()
    end = chips - 1
    give(chips, end, None)
    for s in range(end):
        j = s + 1
        for i in range(2):
            gather(j - 1, i).wait_recv()
            if j < end:
                gather(j, i).start()
        share(j).start()
        keep(j, acc)
        share(j).wait_recv()
        give(chips + j, s, {0: None, 1: end, 2: 0}[s] if chips == 4 else None)

        def take(q, carry, s=s):
            to_peer(s, q).wait_recv()
            part = acc[q] + precv[s, q].astype(jnp.float32)
            if s > 0:
                to_next(s - 1, q).wait_recv()
                part = part + rrecv[s - 1, q].astype(jnp.float32)
            if s > 1:
                to_next(s - 2, q).wait_send()
            ssend[s % 2, q] = part.astype(jnp.bfloat16)
            to_next(s, q).start()
            return carry

        lax.fori_loop(0, parts, take, 0)

    loads[4].wait()
    for q in range(parts):
        cols = slice(q * wide, (q + 1) * wide)
        to_peer(end, q).wait_recv()
        part = last[q] + precv[end, q].astype(jnp.float32)
        to_next(end - 1, q).wait_recv()
        part = part + rrecv[end - 1, q].astype(jnp.float32)
        xbuf[:, cols] = (xbuf[:, cols].astype(jnp.float32) + part.astype(jnp.bfloat16).astype(jnp.float32)).astype(jnp.bfloat16)
    store = pltpu.make_async_copy(xbuf, out, in_sem.at[0])
    store.start()
    for j in range(chips):
        share(j).wait_send()
        if j < end:
            for i in range(2):
                gather(j, i).wait_send()
    for q in range(parts):
        to_peer(1, q).wait_send()
        to_peer(2, q).wait_send()
        for s in (end - 2, end - 1):
            to_next(s, q).wait_send()
    store.wait()


def mlp(tp, hid, mid, w_gate, w_up, w_down):
    rows, d = hid.shape
    ff = w_gate.shape[1]
    parts = 3
    wide = d // parts
    chips = tp // 2
    bf = jnp.bfloat16
    dma = pltpu.SemaphoreType.DMA
    block = lambda n: pltpu.VMEM((n, parts, rows, wide), bf)
    return pl.pallas_call(
        functools.partial(mlp_kernel, tp, parts),
        out_shape=jax.ShapeDtypeStruct((rows, d), bf),
        in_specs=[ANY] * 5,
        out_specs=ANY,
        scratch_shapes=[
            pltpu.VMEM((2 * chips, rows, d), bf),
            pltpu.VMEM((d, ff), bf), pltpu.VMEM((d, ff), bf), pltpu.VMEM((ff, d), bf),
            pltpu.VMEM((rows, d), bf), pltpu.VMEM((rows, ff), bf),
            pltpu.VMEM((parts, rows, wide), jnp.float32), pltpu.VMEM((parts, rows, wide), jnp.float32),
            block(2), block(chips), block(2), block(chips - 1),
            dma((5,)), dma((chips - 1, 2)), dma((chips - 1, 2)), dma((chips,)), dma((chips,)),
            dma((chips, parts)), dma((chips, parts)), dma((chips - 1, parts)), dma((chips - 1, parts)),
        ],
        compiler_params=pltpu.CompilerParams(collective_id=2, has_side_effects=True, vmem_limit_bytes=67043328),
        cost_estimate=cost(1e11, 2e7),
        name="mlp",
    )(hid, mid, w_gate, w_up, w_down)


def solution(mesh):
    tp = mesh.shape['tp']
    row_spec = P(('dp', 'tp'), None)
    group_vec = P('dp')
    table_spec = P('dp', None)
    cache_spec = P('dp', None, 'tp', None)
    col_split = P(None, 'tp')
    row_split = P('tp', None)
    gain_spec = P(None)

    def device_layer(x_in, req_ids, positions, block_table, ctx_len, k_pages, v_pages, w_q, w_k, w_v, w_o, w_gate, w_up, w_down, g_attn, g_mlp):
        pool, page, kv_heads, head = k_pages.shape
        tokens = positions.shape[0]
        n_dec = block_table.shape[0] - 1
        chunk_len = tokens - n_dec
        width = block_table.shape[1]
        pre_pages = width - chunk_len // page
        dec_pages = (pool - width) // n_dec
        n_q = w_q.shape[1] // head

        hidden = lax.all_gather(rms_norm(x_in, g_attn), 'tp', axis=0, tiled=True)
        ko, vo, kd, vd, kc, vc = stage_cache(block_table, req_ids, k_pages.reshape(pool, page, head), v_pages.reshape(pool, page, head), n_dec, dec_pages, pre_pages)
        cos, sin = rope_tables(positions, head)
        w_qkv = jnp.concatenate([w_q, w_k, w_v], axis=1)
        q, kn, vn = qkv(hidden, w_qkv, cos, sin, head)
        chunk_out = chunk_attention(q, kc, vc, kn, vn, chunk_len)
        q_dec = jnp.pad(jnp.transpose(q[:, chunk_len:], (1, 0, 2)), ((0, 0), (0, 8 - n_q), (0, 0)))
        dec_out = decode_attention(positions, q_dec, kd, vd, kn[chunk_len:, None], vn[chunk_len:, None], n_q)
        dec_out = dec_out[:, :n_q].reshape(n_dec, n_q * head)
        ko, vo = update_cache(block_table, req_ids, positions, kn, vn, ko, vo, n_dec, pre_pages)
        attn_rows = jnp.concatenate([chunk_out, dec_out], axis=0)
        mid_rows, hidden_mlp = project(tp, attn_rows.reshape(tp, tokens // tp, n_q * head), w_o, x_in, g_mlp)
        x_out = mlp(tp, hidden_mlp, mid_rows, w_gate, w_up, w_down)
        return x_out, ko.reshape(k_pages.shape), vo.reshape(v_pages.shape)

    return jax.shard_map(device_layer, mesh=mesh, in_specs=(row_spec, group_vec, group_vec, table_spec, group_vec, cache_spec, cache_spec, col_split, col_split, col_split, row_split, col_split, col_split, row_split, gain_spec, gain_spec), out_specs=(row_spec, cache_spec, cache_spec), check_vma=False)
```

```python
import functools

import jax
import jax.numpy as jnp
from jax import lax
from jax.experimental import pallas as pl
from jax.experimental.pallas import tpu as pltpu
from jax.sharding import PartitionSpec as P

EPS = 1e-5
THETA = 500000.0
LOG2E = 1.4426950408889634
ANY = pl.BlockSpec(memory_space=pl.ANY)
SMEM = pl.BlockSpec(memory_space=pltpu.SMEM)
VMEM = pl.BlockSpec(memory_space=pltpu.VMEM)


def cost(flops, nbytes):
    return pl.CostEstimate(flops=int(flops), bytes_accessed=int(nbytes), transcendentals=0)


def ring_places(tp):
    chips = tp // 2
    me = lax.axis_index('tp')
    chip, core = me // 2, lax.rem(me, 2)
    sign = 1 - 2 * core
    peer = 2 * chip + 1 - core

    def chip_at(offset):
        return lax.rem(chip + sign * offset + 2 * chips, chips)

    return chip, core, peer, chip_at


def greet(*others):
    barrier = pltpu.get_barrier_semaphore()
    for other in others:
        pl.semaphore_signal(barrier, inc=1, device_id={'tp': other}, device_id_type=pl.DeviceIdType.MESH)
    pl.semaphore_wait(barrier, len(others))


def remote(src, dst, send, recv, to):
    return pltpu.make_async_remote_copy(src_ref=src, dst_ref=dst, send_sem=send, recv_sem=recv, device_id={'tp': to}, device_id_type=pl.DeviceIdType.MESH)


def front_kernel(tp, x, g, cos, sin, w_q, w_k, w_v, q_out, k_out, v_out,
                 hbuf, w, w_sem, ag_s, ag_r, pg_s, pg_r):
    chips = tp // 2
    chip, core, peer, chip_at = ring_places(tp)
    nxt = 2 * chip_at(1) + core
    prv = 2 * chip_at(-1) + core
    rows, d = x.shape
    n_q = q_out.shape[0]
    head = k_out.shape[2]
    halves = ((0, 144), (144, rows - 144))

    def gather(j, i):
        at = pl.ds(*halves[i])
        return remote(hbuf.at[j, at], hbuf.at[j + 1, at], ag_s.at[j, i], ag_r.at[j, i], nxt)

    def share(j):
        return remote(hbuf.at[j], hbuf.at[chips + j], pg_s.at[j], pg_r.at[j], peer)

    w_cols = n_q * head
    loads = [
        pltpu.make_async_copy(w_q, w.at[:, pl.ds(0, w_cols)], w_sem.at[0]),
        pltpu.make_async_copy(w_k, w.at[:, pl.ds(w_cols, head)], w_sem.at[1]),
        pltpu.make_async_copy(w_v, w.at[:, pl.ds(w_cols + head, head)], w_sem.at[2]),
    ]
    for load in loads:
        load.start()
    rows32 = x[...].astype(jnp.float32)
    inv_rms = lax.rsqrt(jnp.mean(rows32 * rows32, axis=-1, keepdims=True) + EPS)
    hbuf[0] = (rows32 * inv_rms * g[...].astype(jnp.float32)).astype(jnp.bfloat16)
    greet(peer, nxt, prv)
    for i in range(2):
        gather(0, i).start()
    share(0).start()

    def qkv(j, block):
        z = jnp.dot(hbuf[j], w[...], preferred_element_type=jnp.float32).astype(jnp.bfloat16)
        cs, sn = cos[block], sin[block]
        for n in range(n_q + 1):
            part = z[:, n * head:(n + 1) * head].astype(jnp.float32)
            val = (part * cs + pltpu.roll(part, head // 2, 1) * sn).astype(jnp.bfloat16)
            if n < n_q:
                q_out[n, block] = val
            else:
                k_out[block] = val
        v_out[block] = z[:, (n_q + 1) * head:]

    for load in loads:
        load.wait()
    qkv(0, 2 * chip + core)
    share(0).wait_recv()
    qkv(chips, peer)
    for j in range(1, chips):
        for i in range(2):
            gather(j - 1, i).wait_recv()
            if j < chips - 1:
                gather(j, i).start()
        share(j).start()
        qkv(j, 2 * chip_at(-j) + core)
        share(j).wait_recv()
        qkv(chips + j, 2 * chip_at(j) + 1 - core)
    for j in range(chips):
        share(j).wait_send()
        if j < chips - 1:
            for i in range(2):
                gather(j, i).wait_send()


def front(tp, x, g, cos, sin, w_q, w_k, w_v, head):
    rows, d = x.shape
    n_q = w_q.shape[1] // head
    chips = tp // 2
    bf = jnp.bfloat16
    dma = pltpu.SemaphoreType.DMA
    shape = lambda *dims: jax.ShapeDtypeStruct(dims, bf)
    new = shape(tp, rows, head)
    return pl.pallas_call(
        functools.partial(front_kernel, tp),
        out_shape=[shape(n_q, tp, rows, head), new, new],
        in_specs=[VMEM] * 4 + [ANY] * 3,
        out_specs=[VMEM] * 3,
        scratch_shapes=[
            pltpu.VMEM((2 * chips, rows, d), bf),
            pltpu.VMEM((d, (n_q + 2) * head), bf),
            dma((3,)), dma((chips - 1, 2)), dma((chips - 1, 2)), dma((chips,)), dma((chips,)),
        ],
        compiler_params=pltpu.CompilerParams(collective_id=0, has_side_effects=True, vmem_limit_bytes=60 * 2**20),
        cost_estimate=cost(6e10, 1e7),
        name="front",
    )(x, g.reshape(1, d), cos, sin, w_q, w_k, w_v)


def cache_kernel(parts, scale, pre_pages, dec_pages, table, reqs, pos, q, kn, vn, kp, vp, out, ko, vo, kc, vc,
                 kbuf, vbuf, prob, total, qf, of, in_sem, out_sem):
    n_q, n_dec, head = q.shape
    pool, page, _ = kbuf.shape
    step = pool // parts
    chunk_len = reqs.shape[0] - n_dec
    chunk_pages = chunk_len // page
    some = 16
    wide = some * page
    pairs = ((kp, kbuf, ko, kn, kc), (vp, vbuf, vo, vn, vc))

    def copy_in(c, i):
        at = pl.ds(i * step, step)
        return pltpu.make_async_copy(pairs[c][0].at[at], pairs[c][1].at[at], in_sem.at[c, i])

    def copy_out(c, i):
        at = pl.ds(i * step, step)
        return pltpu.make_async_copy(pairs[c][1].at[at], pairs[c][2].at[at], out_sem.at[c, i])

    for c in range(2):
        for i in range(parts):
            copy_in(c, i).start()
    qf[...] = q[...].astype(jnp.float32)
    req0 = reqs[0]

    def arrive(c):
        _, buf, _, new, line = pairs[c]
        for i in range(parts):
            copy_in(c, i).wait()

        def prefix(i, carry):
            line[pl.ds(pl.multiple_of(i * page, page), page), :] = buf[table[req0, i]]
            return carry

        lax.fori_loop(0, pre_pages, prefix, 0, unroll=8)

        def chunk(i, carry):
            rows = new[pl.ds(pl.multiple_of(i * page, page), page), :]
            buf[table[req0, pre_pages + i]] = rows
            line[pl.ds(pl.multiple_of((pre_pages + i) * page, page), page), :] = rows
            return carry

        lax.fori_loop(0, chunk_pages, chunk, 0, unroll=8)
        fresh = new[pl.ds(chunk_len, n_dec), :].astype(jnp.float32)
        of[c] = fresh

        def decode(i, carry):
            p = pos[chunk_len + i]
            at = table[reqs[chunk_len + i], p // page]
            hit = lax.broadcasted_iota(jnp.int32, (page, head), 0) == lax.rem(p, page)
            row = jnp.broadcast_to(of[c, pl.ds(i, 1), :], (page, head))
            buf[at] = jnp.where(hit, row, buf[at].astype(jnp.float32)).astype(jnp.bfloat16)
            return carry

        lax.fori_loop(0, n_dec, decode, 0, unroll=4)
        for i in range(parts):
            copy_out(c, i).start()

    def some_pages(buf, req, t):
        return jnp.concatenate([buf[table[req, t * some + j]] for j in range(some)], axis=0)

    col = lax.broadcasted_iota(jnp.int32, (8, dec_pages * page), 1)
    blank = jnp.zeros((8 - n_q, head), jnp.float32)
    both = 2

    arrive(0)

    def score(g, carry):
        for r in range(both):
            i = g * both + r
            req = reqs[chunk_len + i]
            qr = jnp.concatenate([qf[n, pl.ds(i, 1), :] for n in range(n_q)] + [blank], axis=0).astype(jnp.bfloat16)
            s = jnp.concatenate([
                lax.dot_general(qr, some_pages(kbuf, req, t), (((1,), (1,)), ((), ())), preferred_element_type=jnp.float32)
                for t in range(dec_pages // some)], axis=1)
            s = jnp.where(col <= pos[chunk_len + i], s, -1e30)
            p = jnp.exp2((s - jnp.max(s, axis=-1, keepdims=True)) * scale)
            total[i] = jnp.broadcast_to(jnp.sum(p, axis=-1, keepdims=True), (8, head))
            prob[i] = p
        return carry

    lax.fori_loop(0, n_dec // both, score, 0)
    arrive(1)

    def mix(g, carry):
        for r in range(both):
            i = g * both + r
            req = reqs[chunk_len + i]
            o = sum(
                jnp.dot(prob[i, :, t * wide:(t + 1) * wide].astype(jnp.bfloat16), some_pages(vbuf, req, t), preferred_element_type=jnp.float32)
                for t in range(dec_pages // some))
            o = o / total[i]
            for n in range(n_q):
                of[n, pl.ds(i, 1), :] = o[n:n + 1]
        return carry

    lax.fori_loop(0, n_dec // both, mix, 0)
    for n in range(n_q):
        out[:, n * head:(n + 1) * head] = of[n].astype(jnp.bfloat16)
    for c in range(2):
        for i in range(parts):
            copy_out(c, i).wait()


def cache_and_decode(table, reqs, pos, q, kn, vn, kp, vp, pre_pages, dec_pages):
    n_q, tokens, head = q.shape
    pool, page, _ = kp.shape
    n_dec = table.shape[0] - 1
    parts = 4
    bf, f32 = jnp.bfloat16, jnp.float32
    first = (tokens - n_dec) // n_dec
    full = jax.ShapeDtypeStruct(kp.shape, bf)
    line = jax.ShapeDtypeStruct((table.shape[1] * page, head), bf)
    dma = pltpu.SemaphoreType.DMA
    whole = lambda *dims: pl.BlockSpec(dims, lambda i: (0,) * len(dims))
    return pl.pallas_call(
        functools.partial(cache_kernel, parts, head ** -0.5 * LOG2E, pre_pages, dec_pages),
        grid=(1,),
        out_shape=[jax.ShapeDtypeStruct((n_dec, n_q * head), bf), full, full, line, line],
        in_specs=[SMEM, SMEM, SMEM, pl.BlockSpec((n_q, n_dec, head), lambda i: (0, first, 0)), whole(tokens, head), whole(tokens, head), ANY, ANY],
        out_specs=[whole(n_dec, n_q * head), ANY, ANY, whole(*line.shape), whole(*line.shape)],
        scratch_shapes=[
            pltpu.VMEM(kp.shape, bf), pltpu.VMEM(kp.shape, bf),
            pltpu.VMEM((n_dec, 8, dec_pages * page), f32), pltpu.VMEM((n_dec, 8, head), f32),
            pltpu.VMEM((n_q, n_dec, head), f32), pltpu.VMEM((n_q, n_dec, head), f32),
            dma((2, parts)), dma((2, parts)),
        ],
        compiler_params=pltpu.CompilerParams(vmem_limit_bytes=60 * 2**20),
        cost_estimate=cost(2e10, 1e8),
        name="cache_and_decode",
    )(table, reqs, pos, q, kn, vn, kp, vp)


def rope_tables(positions, head):
    half = head // 2
    lane = jnp.arange(head)
    inv_freq = THETA ** (-(lane % half).astype(jnp.float32) * 2.0 / head)
    angles = positions.astype(jnp.float32)[:, None] * inv_freq[None, :]
    return jnp.cos(angles), jnp.sin(angles) * jnp.where(lane < half, -1.0, 1.0)[None, :]


def attend_kernel(tp, parts, scale, tile, pre_len, q, dec, w_o, x, g, keys, vals, mid_out, hid_out,
                  score, top, weight, acc, o,
                  psend, precv, ssend, rrecv, ps_sem, pr_sem, ss_sem, rr_sem):
    chips = tp // 2
    chip, core, peer, chip_at = ring_places(tp)
    nxt = 2 * chip_at(1) + core
    prv = 2 * chip_at(-1) + core
    n_q, _, rows, head = q.shape
    wide = psend.shape[3]
    span = keys.shape[0]
    pre_tiles, all_tiles = pre_len // tile, span // tile
    n_dec = dec.shape[0]
    greet(peer, nxt, prv)

    def to_peer(s, p):
        return remote(psend.at[lax.rem(s, 2), p], precv.at[s, p], ps_sem.at[s, p], pr_sem.at[s, p], peer)

    def to_next(s, p):
        return remote(ssend.at[s, p], rrecv.at[s, p], ss_sem.at[s, p], rr_sem.at[s, p], nxt)

    def theirs(s):
        return 2 * chip_at(s + 1) + 1 - core

    def mine(s):
        return 2 * chip_at(-(s + 1)) + core

    def tiles(block):
        return jnp.minimum(pre_tiles + ((block + 1) * rows + tile - 1) // tile, all_tiles)

    def lanes(fn, v):
        out = v[:, :head]
        for i in range(1, tile // head):
            out = fn(out, v[:, i * head:(i + 1) * head])
        return out

    def at(t):
        return pl.ds(pl.multiple_of(t * tile, tile), tile)

    def scores(block, slot, t, masked):
        kt = keys[at(t), :]
        if masked:
            diff = lax.broadcasted_iota(jnp.int32, (rows, tile), 1) - lax.broadcasted_iota(jnp.int32, (rows, tile), 0)
            seen = diff <= pre_len + block * rows - t * tile
        for n in range(n_q):
            s = lax.dot_general(q[n, block], kt, (((1,), (1,)), ((), ())), preferred_element_type=jnp.float32)
            if masked:
                s = jnp.where(seen, s, -1e30)
            score[slot, n, :, at(t)] = s
            top[slot, n] = jnp.maximum(top[slot, n], lanes(jnp.maximum, s))

    def mix(slot, t):
        vt = vals[at(t), :]
        for n in range(n_q):
            p = jnp.exp2((score[slot, n, :, at(t)] - top[slot, n, :, :1]) * scale)
            weight[n] += lanes(jnp.add, p)
            acc[n] += jnp.dot(p.astype(jnp.bfloat16), vt, preferred_element_type=jnp.float32)

    def loop(lo, hi, fn):
        def body(t, carry):
            fn(t)
            return carry

        lax.fori_loop(lo, hi, body, 0)

    def run(slot, block, ahead, more):
        other = 1 - slot
        for n in range(n_q):
            top[slot, n] = jnp.broadcast_to(jnp.max(top[slot, n], axis=-1, keepdims=True), (rows, head))
        top[other] = jnp.full(top.shape[1:], -jnp.inf, jnp.float32)
        weight[...] = jnp.zeros_like(weight)
        acc[...] = jnp.zeros_like(acc)
        now = tiles(block)
        then = tiles(ahead) * more
        first = pre_tiles * more

        def both(masked):
            def fn(t):
                scores(ahead, other, t, masked)
                mix(slot, t)
            return fn

        loop(0, first, both(False))
        joint = jnp.maximum(first, jnp.minimum(now, then))
        loop(first, joint, both(True))
        loop(joint, then, lambda t: scores(ahead, other, t, True))
        loop(joint, now, lambda t: mix(slot, t))
        for n in range(n_q):
            total = jnp.sum(weight[n], axis=-1, keepdims=True)
            o[:, n * head:(n + 1) * head] = (acc[n] / total).astype(jnp.bfloat16)

        @pl.when(block == tp - 1)
        def _():
            o[pl.ds(rows - n_dec, n_dec), :] = dec[...]

    def product(p):
        cols = pl.ds(pl.multiple_of(p * wide, wide), wide)
        return jnp.dot(o[...], w_o[:, cols], preferred_element_type=jnp.float32)

    top[0] = jnp.full(top.shape[1:], -jnp.inf, jnp.float32)
    loop(0, tiles(theirs(0)), lambda t: scores(theirs(0), 0, t, True))

    def step(s, carry):
        run(0, theirs(s), mine(s), 1)

        def give(p):
            @pl.when(s > 1)
            def _():
                to_peer(s - 2, p).wait_send()

            psend[lax.rem(s, 2), p] = product(p).astype(jnp.bfloat16)
            to_peer(s, p).start()

        loop(0, parts, give)
        run(1, mine(s), theirs(s + 1), jnp.where(s < chips - 1, 1, 0))

        def take(p):
            own = product(p)
            to_peer(s, p).wait_recv()
            own = own + precv[s, p].astype(jnp.float32)
            cols = pl.ds(pl.multiple_of(p * wide, wide), wide)
            score[1, 0, :, cols] = own

            @pl.when(s > 0)
            def _():
                to_next(s - 1, p).wait_recv()
                score[1, 0, :, cols] = own + rrecv[s - 1, p].astype(jnp.float32)

            @pl.when(s < chips - 1)
            def _():
                ssend[s, p] = score[1, 0, :, cols].astype(jnp.bfloat16)
                to_next(s, p).start()

        loop(0, parts, take)
        return carry

    lax.fori_loop(0, chips, step, 0)

    total = score.at[1, 0]
    square = jnp.zeros((rows, 1), jnp.float32)
    for p in range(parts):
        cols = slice(p * wide, (p + 1) * wide)
        mid = (x[:, cols].astype(jnp.float32) + total[:, cols].astype(jnp.bfloat16).astype(jnp.float32)).astype(jnp.bfloat16)
        mid_out[:, cols] = mid
        mid = mid.astype(jnp.float32)
        total[:, cols] = mid
        square = square + jnp.sum(mid * mid, axis=-1, keepdims=True)
    inv_rms = lax.rsqrt(square / (parts * wide) + EPS)
    for p in range(parts):
        cols = slice(p * wide, (p + 1) * wide)
        hid_out[:, cols] = (total[:, cols] * inv_rms * g[:, cols].astype(jnp.float32)).astype(jnp.bfloat16)
    for p in range(parts):
        for s in range(chips):
            if s >= chips - 2:
                to_peer(s, p).wait_send()
            if s < chips - 1:
                to_next(s, p).wait_send()


def attend_project(tp, q, dec, w_o, x, g, keys, vals, pre_len):
    n_q, tokens, head = q.shape
    rows, d = x.shape
    n_dec = dec.shape[0]
    parts = 3
    wide = d // parts
    chips = tp // 2
    tile = 512
    span = keys.shape[0]
    bf, f32 = jnp.bfloat16, jnp.float32
    dma = pltpu.SemaphoreType.DMA
    block = lambda n: pltpu.VMEM((n, parts, rows, wide), bf)
    out = jax.ShapeDtypeStruct((rows, d), bf)
    return pl.pallas_call(
        functools.partial(attend_kernel, tp, parts, head ** -0.5 * LOG2E, tile, pre_len),
        out_shape=[out, out],
        in_specs=[VMEM] * 7,
        out_specs=[VMEM] * 2,
        scratch_shapes=[
            pltpu.VMEM((2, n_q, rows, span), f32), pltpu.VMEM((2, n_q, rows, head), f32),
            pltpu.VMEM((n_q, rows, head), f32), pltpu.VMEM((n_q, rows, head), f32),
            pltpu.VMEM((rows, n_q * head), bf),
            block(2), block(chips), block(chips - 1), block(chips - 1),
            dma((chips, parts)), dma((chips, parts)), dma((chips - 1, parts)), dma((chips - 1, parts)),
        ],
        compiler_params=pltpu.CompilerParams(collective_id=1, has_side_effects=True, vmem_limit_bytes=67043328),
        cost_estimate=cost(6e10, 1e7),
        name="attend_project",
    )(q.reshape(n_q, tp, rows, head), dec, w_o, x, g.reshape(1, d), keys, vals)


def mlp_kernel(tp, parts, hid, mid, w_gate, w_up, w_down, out,
               hbuf, gbuf, ubuf, dbuf, xbuf, act, acc, last, psend, precv, ssend, rrecv,
               in_sem, ag_s, ag_r, pg_s, pg_r, ps_sem, pr_sem, ss_sem, rr_sem):
    chips = tp // 2
    chip, core, peer, chip_at = ring_places(tp)
    nxt = 2 * chip_at(1) + core
    prv = 2 * chip_at(-1) + core
    _, rows, wide = acc.shape
    ff = gbuf.shape[1]
    tile = 256
    cut = 144
    halves = ((0, cut), (cut, rows - cut))
    loads = [pltpu.make_async_copy(a, b, in_sem.at[i]) for i, (a, b) in enumerate(
        ((hid, hbuf.at[0]), (w_gate, gbuf), (w_up, ubuf), (w_down, dbuf), (mid, xbuf)))]
    for load in loads:
        load.start()
    greet(peer, nxt, prv)

    def gather(j, i):
        first, n = halves[i]
        cut_rows = pl.ds(first, n)
        return remote(hbuf.at[j, cut_rows], hbuf.at[j + 1, cut_rows], ag_s.at[j, i], ag_r.at[j, i], nxt)

    def share(j):
        return remote(hbuf.at[j], hbuf.at[chips + j], pg_s.at[j], pg_r.at[j], peer)

    def to_peer(s, q):
        return remote(psend.at[s % 2, q], precv.at[s, q], ps_sem.at[s, q], pr_sem.at[s, q], peer)

    def to_next(s, q):
        return remote(ssend.at[s % 2, q], rrecv.at[s, q], ss_sem.at[s, q], rr_sem.at[s, q], nxt)

    def hidden_act(j):
        def body(t, carry):
            cols = pl.ds(pl.multiple_of(t * tile, tile), tile)
            gate = jnp.dot(hbuf[j], gbuf[:, cols], preferred_element_type=jnp.float32)
            up = jnp.dot(hbuf[j], ubuf[:, cols], preferred_element_type=jnp.float32)
            act[:, cols] = (gate * jax.nn.sigmoid(gate) * up).astype(jnp.bfloat16)
            return carry

        lax.fori_loop(0, ff // tile, body, 0)

    def down(q):
        cols = pl.ds(pl.multiple_of(q * wide, wide), wide)
        return jnp.dot(act[...], dbuf[:, cols], preferred_element_type=jnp.float32)

    def keep(j, dst):
        hidden_act(j)

        def body(q, carry):
            dst[q] = down(q)
            return carry

        lax.fori_loop(0, parts, body, 0)

    def give(j, s, before):
        hidden_act(j)

        def body(q, carry):
            if before is not None:
                to_peer(before, q).wait_send()
            psend[s % 2, q] = down(q).astype(jnp.bfloat16)
            to_peer(s, q).start()
            return carry

        lax.fori_loop(0, parts, body, 0)

    loads[0].wait()
    for i in range(2):
        gather(0, i).start()
    share(0).start()
    for load in loads[1:4]:
        load.wait()
    keep(0, last)
    share(0).wait_recv()
    end = chips - 1
    give(chips, end, None)
    for s in range(end):
        j = s + 1
        for i in range(2):
            gather(j - 1, i).wait_recv()
            if j < end:
                gather(j, i).start()
        share(j).start()
        keep(j, acc)
        share(j).wait_recv()
        give(chips + j, s, {0: None, 1: end, 2: 0}[s] if chips == 4 else None)

        def take(q, carry, s=s):
            to_peer(s, q).wait_recv()
            part = acc[q] + precv[s, q].astype(jnp.float32)
            if s > 0:
                to_next(s - 1, q).wait_recv()
                part = part + rrecv[s - 1, q].astype(jnp.float32)
            if s > 1:
                to_next(s - 2, q).wait_send()
            ssend[s % 2, q] = part.astype(jnp.bfloat16)
            to_next(s, q).start()
            return carry

        lax.fori_loop(0, parts, take, 0)

    loads[4].wait()
    for q in range(parts):
        cols = slice(q * wide, (q + 1) * wide)
        to_peer(end, q).wait_recv()
        part = last[q] + precv[end, q].astype(jnp.float32)
        to_next(end - 1, q).wait_recv()
        part = part + rrecv[end - 1, q].astype(jnp.float32)
        xbuf[:, cols] = (xbuf[:, cols].astype(jnp.float32) + part.astype(jnp.bfloat16).astype(jnp.float32)).astype(jnp.bfloat16)
    store = pltpu.make_async_copy(xbuf, out, in_sem.at[0])
    store.start()
    for j in range(chips):
        share(j).wait_send()
        if j < end:
            for i in range(2):
                gather(j, i).wait_send()
    for q in range(parts):
        to_peer(1, q).wait_send()
        to_peer(2, q).wait_send()
        for s in (end - 2, end - 1):
            to_next(s, q).wait_send()
    store.wait()


def mlp(tp, hid, mid, w_gate, w_up, w_down):
    rows, d = hid.shape
    ff = w_gate.shape[1]
    parts = 3
    wide = d // parts
    chips = tp // 2
    bf = jnp.bfloat16
    dma = pltpu.SemaphoreType.DMA
    block = lambda n: pltpu.VMEM((n, parts, rows, wide), bf)
    return pl.pallas_call(
        functools.partial(mlp_kernel, tp, parts),
        out_shape=jax.ShapeDtypeStruct((rows, d), bf),
        in_specs=[ANY] * 5,
        out_specs=ANY,
        scratch_shapes=[
            pltpu.VMEM((2 * chips, rows, d), bf),
            pltpu.VMEM((d, ff), bf), pltpu.VMEM((d, ff), bf), pltpu.VMEM((ff, d), bf),
            pltpu.VMEM((rows, d), bf), pltpu.VMEM((rows, ff), bf),
            pltpu.VMEM((parts, rows, wide), jnp.float32), pltpu.VMEM((parts, rows, wide), jnp.float32),
            block(2), block(chips), block(2), block(chips - 1),
            dma((5,)), dma((chips - 1, 2)), dma((chips - 1, 2)), dma((chips,)), dma((chips,)),
            dma((chips, parts)), dma((chips, parts)), dma((chips - 1, parts)), dma((chips - 1, parts)),
        ],
        compiler_params=pltpu.CompilerParams(collective_id=2, has_side_effects=True, vmem_limit_bytes=67043328),
        cost_estimate=cost(1e11, 2e7),
        name="mlp",
    )(hid, mid, w_gate, w_up, w_down)


def solution(mesh):
    tp = mesh.shape['tp']
    row_spec = P(('dp', 'tp'), None)
    group_vec = P('dp')
    table_spec = P('dp', None)
    cache_spec = P('dp', None, 'tp', None)
    col_split = P(None, 'tp')
    row_split = P('tp', None)
    gain_spec = P(None)

    def device_layer(x_in, req_ids, positions, block_table, ctx_len, k_pages, v_pages, w_q, w_k, w_v, w_o, w_gate, w_up, w_down, g_attn, g_mlp):
        pool, page, kv_heads, head = k_pages.shape
        tokens = positions.shape[0]
        n_dec = block_table.shape[0] - 1
        chunk_len = tokens - n_dec
        width = block_table.shape[1]
        pre_pages = width - chunk_len // page
        dec_pages = (pool - width) // n_dec
        n_q = w_q.shape[1] // head

        cos, sin = (t.reshape(tp, tokens // tp, head) for t in rope_tables(positions, head))
        q, kn, vn = front(tp, x_in, g_attn, cos, sin, w_q, w_k, w_v, head)
        q = q.reshape(n_q, tokens, head)
        kn, vn = kn.reshape(tokens, head), vn.reshape(tokens, head)
        dec, ko, vo, keys, vals = cache_and_decode(block_table, req_ids, positions, q, kn, vn, k_pages.reshape(pool, page, head), v_pages.reshape(pool, page, head), pre_pages, dec_pages)
        mid_rows, hidden_mlp = attend_project(tp, q, dec, w_o, x_in, g_mlp, keys, vals, pre_pages * page)
        x_out = mlp(tp, hidden_mlp, mid_rows, w_gate, w_up, w_down)
        return x_out, ko.reshape(k_pages.shape), vo.reshape(v_pages.shape)

    return jax.shard_map(device_layer, mesh=mesh, in_specs=(row_spec, group_vec, group_vec, table_spec, group_vec, cache_spec, cache_spec, col_split, col_split, col_split, row_split, col_split, col_split, row_split, gain_spec, gain_spec), out_specs=(row_spec, cache_spec, cache_spec), check_vma=False)
```

```python
import functools

import jax
import jax.numpy as jnp
import numpy as np
from jax import lax
from jax.experimental import pallas as pl
from jax.experimental.pallas import tpu as pltpu
from jax.sharding import PartitionSpec as P

EPS = 1e-5
THETA = 500000.0
LOG2E = 1.4426950408889634
ANY = pl.BlockSpec(memory_space=pl.ANY)
SMEM = pl.BlockSpec(memory_space=pltpu.SMEM)
VMEM = pl.BlockSpec(memory_space=pltpu.VMEM)


def cost(flops, nbytes):
    return pl.CostEstimate(flops=int(flops), bytes_accessed=int(nbytes), transcendentals=0)


def ring_places(tp):
    chips = tp // 2
    me = lax.axis_index('tp')
    chip, core = me // 2, lax.rem(me, 2)
    sign = 1 - 2 * core
    peer = 2 * chip + 1 - core

    def chip_at(offset):
        return lax.rem(chip + sign * offset + 2 * chips, chips)

    return chip, core, peer, chip_at


def greet(*others):
    barrier = pltpu.get_barrier_semaphore()
    for other in others:
        pl.semaphore_signal(barrier, inc=1, device_id={'tp': other}, device_id_type=pl.DeviceIdType.MESH)
    pl.semaphore_wait(barrier, len(others))


def remote(src, dst, send, recv, to):
    return pltpu.make_async_remote_copy(src_ref=src, dst_ref=dst, send_sem=send, recv_sem=recv, device_id={'tp': to}, device_id_type=pl.DeviceIdType.MESH)


def front_kernel(tp, start, n_dec, pos, x, g, freq, w_q, w_k, w_v, q_out, k_out, v_out,
                 hbuf, w, last_pos, w_sem, ag_s, ag_r, pg_s, pg_r):
    chips = tp // 2
    chip, core, peer, chip_at = ring_places(tp)
    nxt = 2 * chip_at(1) + core
    prv = 2 * chip_at(-1) + core
    rows, d = x.shape
    n_q = q_out.shape[0]
    head = k_out.shape[2]
    halves = ((0, 144), (144, rows - 144))

    def gather(j, i):
        at = pl.ds(*halves[i])
        return remote(hbuf.at[j, at], hbuf.at[j + 1, at], ag_s.at[j, i], ag_r.at[j, i], nxt)

    def share(j, i):
        at = pl.ds(*halves[i])
        return remote(hbuf.at[j, at], hbuf.at[chips + j, at], pg_s.at[j, i], pg_r.at[j, i], peer)

    w_cols = n_q * head
    loads = [
        pltpu.make_async_copy(w_q, w.at[:, pl.ds(0, w_cols)], w_sem.at[0]),
        pltpu.make_async_copy(w_k, w.at[:, pl.ds(w_cols, head)], w_sem.at[1]),
        pltpu.make_async_copy(w_v, w.at[:, pl.ds(w_cols + head, head)], w_sem.at[2]),
    ]
    for load in loads:
        load.start()
    rows32 = x[...].astype(jnp.float32)
    inv_rms = lax.rsqrt(jnp.mean(rows32 * rows32, axis=-1, keepdims=True) + EPS)
    hbuf[0] = (rows32 * inv_rms * g[0:1, :]).astype(jnp.bfloat16)
    greet(peer, nxt, prv)
    for i in range(2):
        gather(0, i).start()
    for i in range(2):
        share(0, i).start()

    def chunk_pos(block):
        return (lax.broadcasted_iota(jnp.int32, (rows, head), 0) + (start + block * rows)).astype(jnp.float32)

    last_pos[...] = chunk_pos(tp - 1)
    first = pos.shape[0] - n_dec

    def note(i, carry):
        last_pos[pl.ds(rows - n_dec + i, 1), :] = jnp.full((1, head), pos[first + i], jnp.int32).astype(jnp.float32)
        return carry

    lax.fori_loop(0, n_dec, note, 0, unroll=8)
    flip = jnp.where(lax.broadcasted_iota(jnp.int32, (1, head), 1) < head // 2, -1.0, 1.0)

    def qkv(j, block, i):
        lo, n = halves[i]
        at = pl.ds(lo, n)
        z = jnp.dot(hbuf[j, at, :], w[...], preferred_element_type=jnp.float32).astype(jnp.bfloat16)
        is_last = jnp.broadcast_to(block, (n, head)) == tp - 1
        angle = jnp.where(is_last, last_pos[at, :], chunk_pos(block)[lo:lo + n]) * freq[...]
        cs, sn = jnp.cos(angle), jnp.sin(angle) * flip
        for m in range(n_q + 1):
            part = z[:, m * head:(m + 1) * head].astype(jnp.float32)
            val = (part * cs + pltpu.roll(part, head // 2, 1) * sn).astype(jnp.bfloat16)
            if m < n_q:
                q_out[m, block, at, :] = val
            else:
                k_out[block, at, :] = val
        v_out[block, at, :] = z[:, (n_q + 1) * head:]

    for load in loads:
        load.wait()
    for i in range(2):
        qkv(0, 2 * chip + core, i)
    for i in range(2):
        share(0, i).wait_recv()
        qkv(chips, peer, i)

    def hop(j, carry):
        for i in range(2):
            gather(j - 1, i).wait_recv()

            @pl.when(j < chips - 1)
            def _():
                gather(j, i).start()

            share(j, i).start()
            qkv(j, 2 * chip_at(-j) + core, i)
            share(j, i).wait_recv()
            qkv(chips + j, 2 * chip_at(j) + 1 - core, i)
        return carry

    lax.fori_loop(1, chips, hop, 0)
    for j in range(chips):
        for i in range(2):
            share(j, i).wait_send()
            if j < chips - 1:
                gather(j, i).wait_send()


def front(tp, pos, x, g, w_q, w_k, w_v, head, n_dec, start):
    rows, d = x.shape
    n_q = w_q.shape[1] // head
    chips = tp // 2
    bf = jnp.bfloat16
    dma = pltpu.SemaphoreType.DMA
    shape = lambda *dims: jax.ShapeDtypeStruct(dims, bf)
    new = shape(tp, rows, head)
    freq = (THETA ** (-(np.arange(head) % (head // 2)) * 2.0 / head)).astype(np.float32)[None, :]
    return pl.pallas_call(
        functools.partial(front_kernel, tp, start, n_dec),
        out_shape=[shape(n_q, tp, rows, head), new, new],
        in_specs=[SMEM] + [VMEM] * 3 + [ANY] * 3,
        out_specs=[VMEM] * 3,
        scratch_shapes=[
            pltpu.VMEM((2 * chips, rows, d), bf),
            pltpu.VMEM((d, (n_q + 2) * head), bf),
            pltpu.VMEM((rows, head), jnp.float32),
            dma((3,)), dma((chips - 1, 2)), dma((chips - 1, 2)), dma((chips, 2)), dma((chips, 2)),
        ],
        compiler_params=pltpu.CompilerParams(collective_id=0, has_side_effects=True, vmem_limit_bytes=60 * 2**20),
        cost_estimate=cost(6e10, 1e7),
        name="front",
    )(pos, x, g, jnp.asarray(freq), w_q, w_k, w_v)


def lanes(fn, v, head):
    out = v[:, :head]
    for i in range(1, v.shape[1] // head):
        out = fn(out, v[:, i * head:(i + 1) * head])
    return out


def tile_at(t, tile):
    return pl.ds(pl.multiple_of(t * tile, tile), tile)


def tile_count(block, rows, pre_len, span, tile):
    return jnp.minimum(pre_len // tile + ((block + 1) * rows + tile - 1) // tile, span // tile)


def tile_scores(q, keys, score, top, block, t, tile, pre_len, masked):
    n_q, _, rows, head = q.shape
    kt = keys[tile_at(t, tile), :]
    if masked:
        diff = lax.broadcasted_iota(jnp.int32, (rows, tile), 1) - lax.broadcasted_iota(jnp.int32, (rows, tile), 0)
        seen = diff <= pre_len + block * rows - t * tile
    for n in range(n_q):
        s = lax.dot_general(q[n, block], kt, (((1,), (1,)), ((), ())), preferred_element_type=jnp.float32)
        if masked:
            s = jnp.where(seen, s, -1e30)
        score[n, :, tile_at(t, tile)] = s
        top[n] = jnp.maximum(top[n], lanes(jnp.maximum, s, head))


def tile_mix(vals, score, top, weight, acc, t, tile, scale):
    n_q, _, head = acc.shape
    vt = vals[tile_at(t, tile), :]
    for n in range(n_q):
        p = jnp.exp2((score[n, :, tile_at(t, tile)] - top[n, :, :1]) * scale)
        weight[n] += lanes(jnp.add, p, head)
        acc[n] += jnp.dot(p.astype(jnp.bfloat16), vt, preferred_element_type=jnp.float32)


def open_mix(top, weight, acc):
    for n in range(top.shape[0]):
        top[n] = jnp.broadcast_to(jnp.max(top[n], axis=-1, keepdims=True), top.shape[1:])
    weight[...] = jnp.zeros_like(weight)
    acc[...] = jnp.zeros_like(acc)


def close_mix(weight, acc, o):
    n_q, _, head = acc.shape
    for n in range(n_q):
        total = jnp.sum(weight[n], axis=-1, keepdims=True)
        o[:, n * head:(n + 1) * head] = (acc[n] / total).astype(jnp.bfloat16)


def loop(lo, hi, fn):
    def body(t, carry):
        fn(t)
        return carry

    lax.fori_loop(lo, hi, body, 0)


def cache_kernel(tp, tile, parts, scale, pre_pages, dec_pages, table, reqs, pos, q, kn, vn, kp, vp, out, ko, vo, kc, vc, early,
                 kbuf, vbuf, prob, total, qf, of, score_buf, top, weight, acc, in_sem, out_sem):
    n_q, n_dec, head = qf.shape
    rows = q.shape[2]
    chip, core, peer, chip_at = ring_places(tp)
    ahead = (2 * chip_at(1) + 1 - core, 2 * chip_at(-1) + core)
    pool, page, _ = kbuf.shape
    step = pool // parts
    chunk_len = reqs.shape[0] - n_dec
    chunk_pages = chunk_len // page
    some = 16
    wide = some * page
    pairs = ((kp, kbuf, ko, kn, kc), (vp, vbuf, vo, vn, vc))

    def copy_in(c, i):
        at = pl.ds(i * step, step)
        return pltpu.make_async_copy(pairs[c][0].at[at], pairs[c][1].at[at], in_sem.at[c, i])

    def copy_out(c, i):
        at = pl.ds(i * step, step)
        return pltpu.make_async_copy(pairs[c][1].at[at], pairs[c][2].at[at], out_sem.at[c, i])

    for c in range(2):
        for i in range(parts):
            copy_in(c, i).start()
    qf[...] = q[:, tp - 1, pl.ds(rows - n_dec, n_dec), :].astype(jnp.float32)
    req0 = reqs[0]

    def arrive(c):
        _, buf, _, new, line = pairs[c]
        for i in range(parts):
            copy_in(c, i).wait()

        def prefix(i, carry):
            line[pl.ds(pl.multiple_of(i * page, page), page), :] = buf[table[req0, i]]
            return carry

        lax.fori_loop(0, pre_pages, prefix, 0, unroll=8)

        def chunk(i, carry):
            rows = new[pl.ds(pl.multiple_of(i * page, page), page), :]
            buf[table[req0, pre_pages + i]] = rows
            line[pl.ds(pl.multiple_of((pre_pages + i) * page, page), page), :] = rows
            return carry

        lax.fori_loop(0, chunk_pages, chunk, 0, unroll=8)
        fresh = new[pl.ds(chunk_len, n_dec), :].astype(jnp.float32)
        of[c] = fresh

        def decode(i, carry):
            p = pos[chunk_len + i]
            at = table[reqs[chunk_len + i], p // page]
            hit = lax.broadcasted_iota(jnp.int32, (page, head), 0) == lax.rem(p, page)
            row = jnp.broadcast_to(of[c, pl.ds(i, 1), :], (page, head))
            buf[at] = jnp.where(hit, row, buf[at].astype(jnp.float32)).astype(jnp.bfloat16)
            return carry

        lax.fori_loop(0, n_dec, decode, 0, unroll=4)
        for i in range(parts):
            copy_out(c, i).start()

    def some_pages(buf, req, t):
        return jnp.concatenate([buf[table[req, t * some + j]] for j in range(some)], axis=0)

    col = lax.broadcasted_iota(jnp.int32, (8, dec_pages * page), 1)
    blank = jnp.zeros((8 - n_q, head), jnp.float32)
    both = 8

    arrive(0)

    def score(g, carry):
        for r in range(both):
            i = g * both + r
            req = reqs[chunk_len + i]
            qr = jnp.concatenate([qf[n, pl.ds(i, 1), :] for n in range(n_q)] + [blank], axis=0).astype(jnp.bfloat16)
            s = jnp.concatenate([
                lax.dot_general(qr, some_pages(kbuf, req, t), (((1,), (1,)), ((), ())), preferred_element_type=jnp.float32)
                for t in range(dec_pages // some)], axis=1)
            s = jnp.where(col <= pos[chunk_len + i], s, -1e30)
            p = jnp.exp2((s - jnp.max(s, axis=-1, keepdims=True)) * scale)
            total[i] = jnp.broadcast_to(jnp.sum(p, axis=-1, keepdims=True), (8, head))
            prob[i] = p
        return carry

    lax.fori_loop(0, n_dec // both, score, 0)
    pre_len = pre_pages * page
    span = kc.shape[0]

    def block_scores(block):
        top[...] = jnp.full(top.shape, -jnp.inf, jnp.float32)
        loop(0, tile_count(block, rows, pre_len, span, tile),
             lambda t: tile_scores(q, kc, score_buf, top, block, t, tile, pre_len, True))

    def block_mix(block, e):
        open_mix(top, weight, acc)
        loop(0, tile_count(block, rows, pre_len, span, tile),
             lambda t: tile_mix(vc, score_buf, top, weight, acc, t, tile, scale))
        close_mix(weight, acc, early.at[e])

    block_scores(ahead[0])
    arrive(1)

    def mix(g, carry):
        for r in range(both):
            i = g * both + r
            req = reqs[chunk_len + i]
            o = sum(
                jnp.dot(prob[i, :, t * wide:(t + 1) * wide].astype(jnp.bfloat16), some_pages(vbuf, req, t), preferred_element_type=jnp.float32)
                for t in range(dec_pages // some))
            o = o / total[i]
            for n in range(n_q):
                of[n, pl.ds(i, 1), :] = o[n:n + 1]
        return carry

    lax.fori_loop(0, n_dec // both, mix, 0)
    for n in range(n_q):
        out[:, n * head:(n + 1) * head] = of[n].astype(jnp.bfloat16)
    block_mix(ahead[0], 0)
    block_scores(ahead[1])
    block_mix(ahead[1], 1)
    for c in range(2):
        for i in range(parts):
            copy_out(c, i).wait()


def cache_and_decode(tp, table, reqs, pos, q, kn, vn, kp, vp, pre_pages, dec_pages, tile):
    n_q, _, rows, head = q.shape
    tokens = tp * rows
    pool, page, _ = kp.shape
    n_dec = table.shape[0] - 1
    parts = 4
    bf, f32 = jnp.bfloat16, jnp.float32
    full = jax.ShapeDtypeStruct(kp.shape, bf)
    line = jax.ShapeDtypeStruct((table.shape[1] * page, head), bf)
    early = jax.ShapeDtypeStruct((2, rows, n_q * head), bf)
    dma = pltpu.SemaphoreType.DMA
    return pl.pallas_call(
        functools.partial(cache_kernel, tp, tile, parts, head ** -0.5 * LOG2E, pre_pages, dec_pages),
        out_shape=[jax.ShapeDtypeStruct((n_dec, n_q * head), bf), full, full, line, line, early],
        in_specs=[SMEM] * 3 + [VMEM] * 3 + [ANY] * 2,
        out_specs=[VMEM, ANY, ANY, VMEM, VMEM, VMEM],
        scratch_shapes=[
            pltpu.VMEM(kp.shape, bf), pltpu.VMEM(kp.shape, bf),
            pltpu.VMEM((n_dec, 8, dec_pages * page), f32), pltpu.VMEM((n_dec, 8, head), f32),
            pltpu.VMEM((n_q, n_dec, head), f32), pltpu.VMEM((n_q, n_dec, head), f32),
            pltpu.VMEM((n_q, rows, line.shape[0]), f32), pltpu.VMEM((n_q, rows, head), f32),
            pltpu.VMEM((n_q, rows, head), f32), pltpu.VMEM((n_q, rows, head), f32),
            dma((2, parts)), dma((2, parts)),
        ],
        compiler_params=pltpu.CompilerParams(vmem_limit_bytes=67043328),
        cost_estimate=cost(4e10, 1e8),
        name="cache_and_decode",
    )(table, reqs, pos, q, kn, vn, kp, vp)


def attend_kernel(tp, parts, scale, tile, pre_len, q, dec, early, w_o_any, x_any, g, keys, vals, mid_out, hid_out,
                  w_o, x, in_sem, score, top, weight, acc, o,
                  psend, precv, ssend, rrecv, ps_sem, pr_sem, ss_sem, rr_sem):
    chips = tp // 2
    chip, core, peer, chip_at = ring_places(tp)
    nxt = 2 * chip_at(1) + core
    prv = 2 * chip_at(-1) + core
    n_q, _, rows, head = q.shape
    wide = psend.shape[3]
    span = keys.shape[0]
    pre_tiles, all_tiles = pre_len // tile, span // tile
    n_dec = dec.shape[0]
    loads = [pltpu.make_async_copy(w_o_any, w_o, in_sem.at[0]), pltpu.make_async_copy(x_any, x, in_sem.at[1])]
    for load in loads:
        load.start()
    greet(peer, nxt, prv)

    def to_peer(s, p):
        return remote(psend.at[lax.rem(s, 2), p], precv.at[s, p], ps_sem.at[s, p], pr_sem.at[s, p], peer)

    def to_next(s, p):
        return remote(ssend.at[s, p], rrecv.at[s, p], ss_sem.at[s, p], rr_sem.at[s, p], nxt)

    def theirs(s):
        return 2 * chip_at(s + 1) + 1 - core

    def mine(s):
        return 2 * chip_at(-(s + 1)) + core

    def tiles(block):
        return tile_count(block, rows, pre_len, span, tile)

    def scores(block, slot, t, masked):
        tile_scores(q, keys, score.at[slot], top.at[slot], block, t, tile, pre_len, masked)

    def mix(slot, t):
        tile_mix(vals, score.at[slot], top.at[slot], weight, acc, t, tile, scale)

    def finish(block):
        @pl.when(block == tp - 1)
        def _():
            o[pl.ds(rows - n_dec, n_dec), :] = dec[...]

    def run(slot, block, ahead, more):
        other = 1 - slot
        open_mix(top.at[slot], weight, acc)
        top[other] = jnp.full(top.shape[1:], -jnp.inf, jnp.float32)
        now = tiles(block)
        then = tiles(ahead) * more
        first = pre_len // tile * more

        def both(masked):
            def fn(t):
                scores(ahead, other, t, masked)
                mix(slot, t)
            return fn

        loop(0, first, both(False))
        joint = jnp.maximum(first, jnp.minimum(now, then))
        loop(first, joint, both(True))
        loop(joint, then, lambda t: scores(ahead, other, t, True))
        loop(joint, now, lambda t: mix(slot, t))
        close_mix(weight, acc, o)
        finish(block)

    def product(p):
        cols = pl.ds(pl.multiple_of(p * wide, wide), wide)
        return jnp.dot(o[...], w_o[:, cols], preferred_element_type=jnp.float32)

    def give_all(s):
        def give(p):
            @pl.when(s > 1)
            def _():
                to_peer(s - 2, p).wait_send()

            psend[lax.rem(s, 2), p] = product(p).astype(jnp.bfloat16)
            to_peer(s, p).start()

        loop(0, parts, give)

    def take_all(s):
        def take(p):
            own = product(p)
            to_peer(s, p).wait_recv()
            own = own + precv[s, p].astype(jnp.float32)
            cols = pl.ds(pl.multiple_of(p * wide, wide), wide)
            score[1, 0, :, cols] = own

            @pl.when(s > 0)
            def _():
                to_next(s - 1, p).wait_recv()
                score[1, 0, :, cols] = own + rrecv[s - 1, p].astype(jnp.float32)

            @pl.when(s < chips - 1)
            def _():
                ssend[s, p] = score[1, 0, :, cols].astype(jnp.bfloat16)
                to_next(s, p).start()

        loop(0, parts, take)

    def step(s, carry):
        @pl.when(s == 0)
        def _():
            o[...] = early[0]
            finish(theirs(0))

        @pl.when(s > 0)
        def _():
            run(0, theirs(s), mine(s), 1)

        give_all(s)

        @pl.when(s == 0)
        def _():
            o[...] = early[1]
            finish(mine(0))

        @pl.when(s > 0)
        def _():
            run(1, mine(s), theirs(s + 1), jnp.where(s < chips - 1, 1, 0))

        take_all(s)

        @pl.when(s == 0)
        def _():
            top[0] = jnp.full(top.shape[1:], -jnp.inf, jnp.float32)
            loop(0, tiles(theirs(1)), lambda t: scores(theirs(1), 0, t, True))

        return carry

    for load in loads:
        load.wait()
    lax.fori_loop(0, chips, step, 0)

    total = score.at[1, 0]
    square = jnp.zeros((rows, 1), jnp.float32)
    for p in range(parts):
        cols = slice(p * wide, (p + 1) * wide)
        mid = (x[:, cols].astype(jnp.float32) + total[:, cols].astype(jnp.bfloat16).astype(jnp.float32)).astype(jnp.bfloat16)
        mid_out[:, cols] = mid
        mid = mid.astype(jnp.float32)
        total[:, cols] = mid
        square = square + jnp.sum(mid * mid, axis=-1, keepdims=True)
    inv_rms = lax.rsqrt(square / (parts * wide) + EPS)
    for p in range(parts):
        cols = slice(p * wide, (p + 1) * wide)
        hid_out[:, cols] = (total[:, cols] * inv_rms * g[1:2, cols]).astype(jnp.bfloat16)
    for p in range(parts):
        for s in range(chips):
            if s >= chips - 2:
                to_peer(s, p).wait_send()
            if s < chips - 1:
                to_next(s, p).wait_send()


def attend_project(tp, q, dec, early, w_o, x, g, keys, vals, pre_len, tile):
    n_q, _, rows, head = q.shape
    d = x.shape[1]
    parts = 3
    wide = d // parts
    chips = tp // 2
    span = keys.shape[0]
    bf, f32 = jnp.bfloat16, jnp.float32
    dma = pltpu.SemaphoreType.DMA
    block = lambda n: pltpu.VMEM((n, parts, rows, wide), bf)
    out = jax.ShapeDtypeStruct((rows, d), bf)
    return pl.pallas_call(
        functools.partial(attend_kernel, tp, parts, head ** -0.5 * LOG2E, tile, pre_len),
        out_shape=[out, out],
        in_specs=[VMEM] * 3 + [ANY] * 2 + [VMEM] * 3,
        out_specs=[VMEM] * 2,
        scratch_shapes=[
            pltpu.VMEM(w_o.shape, bf), pltpu.VMEM((rows, d), bf), dma((2,)),
            pltpu.VMEM((2, n_q, rows, span), f32), pltpu.VMEM((2, n_q, rows, head), f32),
            pltpu.VMEM((n_q, rows, head), f32), pltpu.VMEM((n_q, rows, head), f32),
            pltpu.VMEM((rows, n_q * head), bf),
            block(2), block(chips), block(chips - 1), block(chips - 1),
            dma((chips, parts)), dma((chips, parts)), dma((chips - 1, parts)), dma((chips - 1, parts)),
        ],
        compiler_params=pltpu.CompilerParams(collective_id=1, has_side_effects=True, vmem_limit_bytes=67043328),
        cost_estimate=cost(6e10, 1e7),
        name="attend_project",
    )(q, dec, early, w_o, x, g, keys, vals)


def mlp_kernel(tp, parts, hid, mid, w_gate, w_up, w_down, out,
               hbuf, gbuf, ubuf, dbuf, xbuf, act, acc, last, psend, precv, ssend, rrecv,
               in_sem, ag_s, ag_r, pg_s, pg_r, ps_sem, pr_sem, ss_sem, rr_sem):
    chips = tp // 2
    chip, core, peer, chip_at = ring_places(tp)
    nxt = 2 * chip_at(1) + core
    prv = 2 * chip_at(-1) + core
    _, rows, wide = acc.shape
    ff = gbuf.shape[1]
    tile = 256
    cut = 144
    halves = ((0, cut), (cut, rows - cut))
    loads = [pltpu.make_async_copy(a, b, in_sem.at[i]) for i, (a, b) in enumerate(
        ((hid, hbuf.at[0]), (w_gate, gbuf), (w_up, ubuf), (w_down, dbuf), (mid, xbuf)))]
    for load in loads:
        load.start()
    greet(peer, nxt, prv)

    def gather(j, i):
        first, n = halves[i]
        cut_rows = pl.ds(first, n)
        return remote(hbuf.at[j, cut_rows], hbuf.at[j + 1, cut_rows], ag_s.at[j, i], ag_r.at[j, i], nxt)

    def share(j):
        return remote(hbuf.at[j], hbuf.at[chips + j], pg_s.at[j], pg_r.at[j], peer)

    def to_peer(s, q):
        return remote(psend.at[s % 2, q], precv.at[s, q], ps_sem.at[s, q], pr_sem.at[s, q], peer)

    def to_next(s, q):
        return remote(ssend.at[s % 2, q], rrecv.at[s, q], ss_sem.at[s, q], rr_sem.at[s, q], nxt)

    def hidden_act(j):
        def body(t, carry):
            cols = pl.ds(pl.multiple_of(t * tile, tile), tile)
            gate = jnp.dot(hbuf[j], gbuf[:, cols], preferred_element_type=jnp.float32)
            up = jnp.dot(hbuf[j], ubuf[:, cols], preferred_element_type=jnp.float32)
            act[:, cols] = (gate * jax.nn.sigmoid(gate) * up).astype(jnp.bfloat16)
            return carry

        lax.fori_loop(0, ff // tile, body, 0)

    def down(q):
        cols = pl.ds(pl.multiple_of(q * wide, wide), wide)
        return jnp.dot(act[...], dbuf[:, cols], preferred_element_type=jnp.float32)

    def keep(j, dst):
        hidden_act(j)

        def body(q, carry):
            dst[q] = down(q)
            return carry

        lax.fori_loop(0, parts, body, 0)

    def give(j, s, before):
        hidden_act(j)

        def body(q, carry):
            if before is not None:
                to_peer(before, q).wait_send()
            psend[s % 2, q] = down(q).astype(jnp.bfloat16)
            to_peer(s, q).start()
            return carry

        lax.fori_loop(0, parts, body, 0)

    loads[0].wait()
    for i in range(2):
        gather(0, i).start()
    share(0).start()
    for load in loads[1:4]:
        load.wait()
    keep(0, last)
    share(0).wait_recv()
    end = chips - 1
    give(chips, end, None)
    for s in range(end):
        j = s + 1
        for i in range(2):
            gather(j - 1, i).wait_recv()
            if j < end:
                gather(j, i).start()
        share(j).start()
        keep(j, acc)
        share(j).wait_recv()
        give(chips + j, s, {0: None, 1: end, 2: 0}[s] if chips == 4 else None)

        def take(q, carry, s=s):
            to_peer(s, q).wait_recv()
            part = acc[q] + precv[s, q].astype(jnp.float32)
            if s > 0:
                to_next(s - 1, q).wait_recv()
                part = part + rrecv[s - 1, q].astype(jnp.float32)
            if s > 1:
                to_next(s - 2, q).wait_send()
            ssend[s % 2, q] = part.astype(jnp.bfloat16)
            to_next(s, q).start()
            return carry

        lax.fori_loop(0, parts, take, 0)

    loads[4].wait()
    for q in range(parts):
        cols = slice(q * wide, (q + 1) * wide)
        to_peer(end, q).wait_recv()
        part = last[q] + precv[end, q].astype(jnp.float32)
        to_next(end - 1, q).wait_recv()
        part = part + rrecv[end - 1, q].astype(jnp.float32)
        xbuf[:, cols] = (xbuf[:, cols].astype(jnp.float32) + part.astype(jnp.bfloat16).astype(jnp.float32)).astype(jnp.bfloat16)
    store = pltpu.make_async_copy(xbuf, out, in_sem.at[0])
    store.start()
    for j in range(chips):
        share(j).wait_send()
        if j < end:
            for i in range(2):
                gather(j, i).wait_send()
    for q in range(parts):
        to_peer(1, q).wait_send()
        to_peer(2, q).wait_send()
        for s in (end - 2, end - 1):
            to_next(s, q).wait_send()
    store.wait()


def mlp(tp, hid, mid, w_gate, w_up, w_down):
    rows, d = hid.shape
    ff = w_gate.shape[1]
    parts = 3
    wide = d // parts
    chips = tp // 2
    bf = jnp.bfloat16
    dma = pltpu.SemaphoreType.DMA
    block = lambda n: pltpu.VMEM((n, parts, rows, wide), bf)
    return pl.pallas_call(
        functools.partial(mlp_kernel, tp, parts),
        out_shape=jax.ShapeDtypeStruct((rows, d), bf),
        in_specs=[ANY] * 5,
        out_specs=ANY,
        scratch_shapes=[
            pltpu.VMEM((2 * chips, rows, d), bf),
            pltpu.VMEM((d, ff), bf), pltpu.VMEM((d, ff), bf), pltpu.VMEM((ff, d), bf),
            pltpu.VMEM((rows, d), bf), pltpu.VMEM((rows, ff), bf),
            pltpu.VMEM((parts, rows, wide), jnp.float32), pltpu.VMEM((parts, rows, wide), jnp.float32),
            block(2), block(chips), block(2), block(chips - 1),
            dma((5,)), dma((chips - 1, 2)), dma((chips - 1, 2)), dma((chips,)), dma((chips,)),
            dma((chips, parts)), dma((chips, parts)), dma((chips - 1, parts)), dma((chips - 1, parts)),
        ],
        compiler_params=pltpu.CompilerParams(collective_id=2, has_side_effects=True, vmem_limit_bytes=67043328),
        cost_estimate=cost(1e11, 2e7),
        name="mlp",
    )(hid, mid, w_gate, w_up, w_down)


def solution(mesh):
    tp = mesh.shape['tp']
    row_spec = P(('dp', 'tp'), None)
    group_vec = P('dp')
    table_spec = P('dp', None)
    cache_spec = P('dp', None, 'tp', None)
    col_split = P(None, 'tp')
    row_split = P('tp', None)
    gain_spec = P(None)

    def device_layer(x_in, req_ids, positions, block_table, ctx_len, k_pages, v_pages, w_q, w_k, w_v, w_o, w_gate, w_up, w_down, g_attn, g_mlp):
        pool, page, kv_heads, head = k_pages.shape
        tokens = positions.shape[0]
        n_dec = block_table.shape[0] - 1
        chunk_len = tokens - n_dec
        width = block_table.shape[1]
        pre_pages = width - chunk_len // page
        dec_pages = (pool - width) // n_dec
        n_q = w_q.shape[1] // head

        gains = jnp.stack([g_attn, g_mlp]).astype(jnp.float32)
        q, kn, vn = front(tp, positions, x_in, gains, w_q, w_k, w_v, head, n_dec, pre_pages * page)
        kn, vn = kn.reshape(tokens, head), vn.reshape(tokens, head)
        tile = 512
        dec, ko, vo, keys, vals, early = cache_and_decode(tp, block_table, req_ids, positions, q, kn, vn, k_pages.reshape(pool, page, head), v_pages.reshape(pool, page, head), pre_pages, dec_pages, tile)
        mid_rows, hidden_mlp = attend_project(tp, q, dec, early, w_o, x_in, gains, keys, vals, pre_pages * page, tile)
        x_out = mlp(tp, hidden_mlp, mid_rows, w_gate, w_up, w_down)
        return x_out, ko.reshape(k_pages.shape), vo.reshape(v_pages.shape)

    return jax.shard_map(device_layer, mesh=mesh, in_specs=(row_spec, group_vec, group_vec, table_spec, group_vec, cache_spec, cache_spec, col_split, col_split, col_split, row_split, col_split, col_split, row_split, gain_spec, gain_spec), out_specs=(row_spec, cache_spec, cache_spec), check_vma=False)
```

```python
import functools

import jax
import jax.numpy as jnp
import numpy as np
from jax import lax
from jax.experimental import pallas as pl
from jax.experimental.pallas import tpu as pltpu
from jax.sharding import PartitionSpec as P

EPS = 1e-5
THETA = 500000.0
LOG2E = 1.4426950408889634
ANY = pl.BlockSpec(memory_space=pl.ANY)
SMEM = pl.BlockSpec(memory_space=pltpu.SMEM)
VMEM = pl.BlockSpec(memory_space=pltpu.VMEM)


def cost(flops, nbytes):
    return pl.CostEstimate(flops=int(flops), bytes_accessed=int(nbytes), transcendentals=0)


def ring_places(tp):
    chips = tp // 2
    me = lax.axis_index('tp')
    chip, core = me // 2, lax.rem(me, 2)
    sign = 1 - 2 * core
    peer = 2 * chip + 1 - core

    def chip_at(offset):
        return lax.rem(chip + sign * offset + 2 * chips, chips)

    return chip, core, peer, chip_at


def greet(*others):
    barrier = pltpu.get_barrier_semaphore()
    for other in others:
        pl.semaphore_signal(barrier, inc=1, device_id={'tp': other}, device_id_type=pl.DeviceIdType.MESH)
    pl.semaphore_wait(barrier, len(others))


def remote(src, dst, send, recv, to):
    return pltpu.make_async_remote_copy(src_ref=src, dst_ref=dst, send_sem=send, recv_sem=recv, device_id={'tp': to}, device_id_type=pl.DeviceIdType.MESH)


def front_kernel(tp, start, n_dec, pos, x, g, freq, w_q, w_k, w_v, q_out, k_out, v_out,
                 hbuf, w, last_pos, w_sem, ag_s, ag_r, pg_s, pg_r):
    chips = tp // 2
    chip, core, peer, chip_at = ring_places(tp)
    nxt = 2 * chip_at(1) + core
    prv = 2 * chip_at(-1) + core
    rows, d = x.shape
    n_q = q_out.shape[0]
    head = k_out.shape[2]
    halves = ((0, 144), (144, rows - 144))

    def gather(j, i):
        at = pl.ds(*halves[i])
        return remote(hbuf.at[j, at], hbuf.at[j + 1, at], ag_s.at[j, i], ag_r.at[j, i], nxt)

    def share(j, i):
        at = pl.ds(*halves[i])
        return remote(hbuf.at[j, at], hbuf.at[chips + j, at], pg_s.at[j, i], pg_r.at[j, i], peer)

    w_cols = n_q * head
    loads = [
        pltpu.make_async_copy(w_q, w.at[:, pl.ds(0, w_cols)], w_sem.at[0]),
        pltpu.make_async_copy(w_k, w.at[:, pl.ds(w_cols, head)], w_sem.at[1]),
        pltpu.make_async_copy(w_v, w.at[:, pl.ds(w_cols + head, head)], w_sem.at[2]),
    ]
    for load in loads:
        load.start()
    rows32 = x[...].astype(jnp.float32)
    inv_rms = lax.rsqrt(jnp.mean(rows32 * rows32, axis=-1, keepdims=True) + EPS)
    hbuf[0] = (rows32 * inv_rms * g[0:1, :]).astype(jnp.bfloat16)
    greet(peer, nxt, prv)
    for i in range(2):
        gather(0, i).start()
    for i in range(2):
        share(0, i).start()

    def chunk_pos(block):
        return (lax.broadcasted_iota(jnp.int32, (rows, head), 0) + (start + block * rows)).astype(jnp.float32)

    last_pos[...] = chunk_pos(tp - 1)
    first = pos.shape[0] - n_dec

    def note(i, carry):
        last_pos[pl.ds(rows - n_dec + i, 1), :] = jnp.full((1, head), pos[first + i], jnp.int32).astype(jnp.float32)
        return carry

    lax.fori_loop(0, n_dec, note, 0, unroll=8)
    flip = jnp.where(lax.broadcasted_iota(jnp.int32, (1, head), 1) < head // 2, -1.0, 1.0)

    def qkv(j, block, i):
        lo, n = halves[i]
        at = pl.ds(lo, n)
        z = jnp.dot(hbuf[j, at, :], w[...], preferred_element_type=jnp.float32).astype(jnp.bfloat16)
        is_last = jnp.broadcast_to(block, (n, head)) == tp - 1
        angle = jnp.where(is_last, last_pos[at, :], chunk_pos(block)[lo:lo + n]) * freq[...]
        cs, sn = jnp.cos(angle), jnp.sin(angle) * flip
        for m in range(n_q + 1):
            part = z[:, m * head:(m + 1) * head].astype(jnp.float32)
            val = (part * cs + pltpu.roll(part, head // 2, 1) * sn).astype(jnp.bfloat16)
            if m < n_q:
                q_out[m, block, at, :] = val
            else:
                k_out[block, at, :] = val
        v_out[block, at, :] = z[:, (n_q + 1) * head:]

    for load in loads:
        load.wait()
    for i in range(2):
        qkv(0, 2 * chip + core, i)
    for i in range(2):
        share(0, i).wait_recv()
        qkv(chips, peer, i)

    def hop(j, carry):
        for i in range(2):
            gather(j - 1, i).wait_recv()

            @pl.when(j < chips - 1)
            def _():
                gather(j, i).start()

            share(j, i).start()
            qkv(j, 2 * chip_at(-j) + core, i)
            share(j, i).wait_recv()
            qkv(chips + j, 2 * chip_at(j) + 1 - core, i)
        return carry

    lax.fori_loop(1, chips, hop, 0)
    for j in range(chips):
        for i in range(2):
            share(j, i).wait_send()
            if j < chips - 1:
                gather(j, i).wait_send()


def front(tp, pos, x, g, w_q, w_k, w_v, head, n_dec, start):
    rows, d = x.shape
    n_q = w_q.shape[1] // head
    chips = tp // 2
    bf = jnp.bfloat16
    dma = pltpu.SemaphoreType.DMA
    shape = lambda *dims: jax.ShapeDtypeStruct(dims, bf)
    new = shape(tp, rows, head)
    freq = (THETA ** (-(np.arange(head) % (head // 2)) * 2.0 / head)).astype(np.float32)[None, :]
    return pl.pallas_call(
        functools.partial(front_kernel, tp, start, n_dec),
        out_shape=[shape(n_q, tp, rows, head), new, new],
        in_specs=[SMEM] + [VMEM] * 3 + [ANY] * 3,
        out_specs=[VMEM] * 3,
        scratch_shapes=[
            pltpu.VMEM((2 * chips, rows, d), bf),
            pltpu.VMEM((d, (n_q + 2) * head), bf),
            pltpu.VMEM((rows, head), jnp.float32),
            dma((3,)), dma((chips - 1, 2)), dma((chips - 1, 2)), dma((chips, 2)), dma((chips, 2)),
        ],
        compiler_params=pltpu.CompilerParams(collective_id=0, has_side_effects=True, vmem_limit_bytes=60 * 2**20),
        cost_estimate=cost(6e10, 1e7),
        name="front",
    )(pos, x, g, jnp.asarray(freq), w_q, w_k, w_v)


def lanes(fn, v, head):
    out = v[:, :head]
    for i in range(1, v.shape[1] // head):
        out = fn(out, v[:, i * head:(i + 1) * head])
    return out


def tile_at(t, tile):
    return pl.ds(pl.multiple_of(t * tile, tile), tile)


def tile_count(block, rows, pre_len, span, tile):
    return jnp.minimum(pre_len // tile + ((block + 1) * rows + tile - 1) // tile, span // tile)


def tile_scores(q, keys, score, top, block, t, tile, pre_len, masked):
    n_q, _, rows, head = q.shape
    kt = keys[tile_at(t, tile), :]
    if masked:
        diff = lax.broadcasted_iota(jnp.int32, (rows, tile), 1) - lax.broadcasted_iota(jnp.int32, (rows, tile), 0)
        seen = diff <= pre_len + block * rows - t * tile
    for n in range(n_q):
        s = lax.dot_general(q[n, block], kt, (((1,), (1,)), ((), ())), preferred_element_type=jnp.float32)
        if masked:
            s = jnp.where(seen, s, -1e30)
        score[n, :, tile_at(t, tile)] = s
        top[n] = jnp.maximum(top[n], lanes(jnp.maximum, s, head))


def tile_mix(vals, score, top, weight, acc, t, tile, scale):
    n_q, _, head = acc.shape
    vt = vals[tile_at(t, tile), :]
    for n in range(n_q):
        p = jnp.exp2((score[n, :, tile_at(t, tile)] - top[n, :, :1]) * scale)
        weight[n] += lanes(jnp.add, p, head)
        acc[n] += jnp.dot(p.astype(jnp.bfloat16), vt, preferred_element_type=jnp.float32)


def open_mix(top, weight, acc):
    for n in range(top.shape[0]):
        top[n] = jnp.broadcast_to(jnp.max(top[n], axis=-1, keepdims=True), top.shape[1:])
    weight[...] = jnp.zeros_like(weight)
    acc[...] = jnp.zeros_like(acc)


def close_mix(weight, acc, o):
    n_q, _, head = acc.shape
    for n in range(n_q):
        total = jnp.sum(weight[n], axis=-1, keepdims=True)
        o[:, n * head:(n + 1) * head] = (acc[n] / total).astype(jnp.bfloat16)


def loop(lo, hi, fn):
    def body(t, carry):
        fn(t)
        return carry

    lax.fori_loop(lo, hi, body, 0)


def cache_kernel(tp, tile, parts, scale, pre_pages, dec_pages, table, reqs, pos, q, kn, vn, kp, vp, out, ko, vo, kc, vc, early,
                 kbuf, vbuf, prob, total, qf, of, score_buf, top, weight, acc, in_sem, out_sem):
    n_q, n_dec, head = qf.shape
    rows = q.shape[2]
    chip, core, peer, chip_at = ring_places(tp)
    ahead = (2 * chip_at(1) + 1 - core, 2 * chip_at(-1) + core)
    pool, page, _ = kbuf.shape
    step = pool // parts
    chunk_len = reqs.shape[0] - n_dec
    chunk_pages = chunk_len // page
    some = 16
    wide = some * page
    pairs = ((kp, kbuf, ko, kn, kc), (vp, vbuf, vo, vn, vc))

    def copy_in(c, i):
        at = pl.ds(i * step, step)
        return pltpu.make_async_copy(pairs[c][0].at[at], pairs[c][1].at[at], in_sem.at[c, i])

    def copy_out(c, i):
        at = pl.ds(i * step, step)
        return pltpu.make_async_copy(pairs[c][1].at[at], pairs[c][2].at[at], out_sem.at[c, i])

    for c in range(2):
        for i in range(parts):
            copy_in(c, i).start()
    qf[...] = q[:, tp - 1, pl.ds(rows - n_dec, n_dec), :].astype(jnp.float32)
    req0 = reqs[0]

    def arrive(c):
        _, buf, _, new, line = pairs[c]
        for i in range(parts):
            copy_in(c, i).wait()
        if c == 1:
            for i in range(parts):
                copy_out(0, i).start()

        def prefix(i, carry):
            line[pl.ds(pl.multiple_of(i * page, page), page), :] = buf[table[req0, i]]
            return carry

        lax.fori_loop(0, pre_pages, prefix, 0, unroll=8)

        def chunk(i, carry):
            rows = new[pl.ds(pl.multiple_of(i * page, page), page), :]
            buf[table[req0, pre_pages + i]] = rows
            line[pl.ds(pl.multiple_of((pre_pages + i) * page, page), page), :] = rows
            return carry

        lax.fori_loop(0, chunk_pages, chunk, 0, unroll=8)
        fresh = new[pl.ds(chunk_len, n_dec), :].astype(jnp.float32)
        of[c] = fresh

        def decode(i, carry):
            p = pos[chunk_len + i]
            at = table[reqs[chunk_len + i], p // page]
            hit = lax.broadcasted_iota(jnp.int32, (page, head), 0) == lax.rem(p, page)
            row = jnp.broadcast_to(of[c, pl.ds(i, 1), :], (page, head))
            buf[at] = jnp.where(hit, row, buf[at].astype(jnp.float32)).astype(jnp.bfloat16)
            return carry

        lax.fori_loop(0, n_dec, decode, 0, unroll=4)
        if c == 1:
            for i in range(parts):
                copy_out(1, i).start()

    def some_pages(buf, req, t):
        return jnp.concatenate([buf[table[req, t * some + j]] for j in range(some)], axis=0)

    col = lax.broadcasted_iota(jnp.int32, (8, dec_pages * page), 1)
    blank = jnp.zeros((8 - n_q, head), jnp.float32)
    both = 8

    arrive(0)

    def score(g, carry):
        for r in range(both):
            i = g * both + r
            req = reqs[chunk_len + i]
            qr = jnp.concatenate([qf[n, pl.ds(i, 1), :] for n in range(n_q)] + [blank], axis=0).astype(jnp.bfloat16)
            s = jnp.concatenate([
                lax.dot_general(qr, some_pages(kbuf, req, t), (((1,), (1,)), ((), ())), preferred_element_type=jnp.float32)
                for t in range(dec_pages // some)], axis=1)
            s = jnp.where(col <= pos[chunk_len + i], s, -1e30)
            p = jnp.exp2((s - jnp.max(s, axis=-1, keepdims=True)) * scale)
            total[i] = jnp.broadcast_to(jnp.sum(p, axis=-1, keepdims=True), (8, head))
            prob[i] = p
        return carry

    lax.fori_loop(0, n_dec // both, score, 0)
    pre_len = pre_pages * page
    span = kc.shape[0]

    def block_scores(block):
        top[...] = jnp.full(top.shape, -jnp.inf, jnp.float32)
        loop(0, tile_count(block, rows, pre_len, span, tile),
             lambda t: tile_scores(q, kc, score_buf, top, block, t, tile, pre_len, True))

    def block_mix(block, e):
        open_mix(top, weight, acc)
        loop(0, tile_count(block, rows, pre_len, span, tile),
             lambda t: tile_mix(vc, score_buf, top, weight, acc, t, tile, scale))
        close_mix(weight, acc, early.at[e])

    arrive(1)

    def mix(g, carry):
        for r in range(both):
            i = g * both + r
            req = reqs[chunk_len + i]
            o = sum(
                jnp.dot(prob[i, :, t * wide:(t + 1) * wide].astype(jnp.bfloat16), some_pages(vbuf, req, t), preferred_element_type=jnp.float32)
                for t in range(dec_pages // some))
            o = o / total[i]
            for n in range(n_q):
                of[n, pl.ds(i, 1), :] = o[n:n + 1]
        return carry

    lax.fori_loop(0, n_dec // both, mix, 0)
    for n in range(n_q):
        out[:, n * head:(n + 1) * head] = of[n].astype(jnp.bfloat16)
    block_scores(ahead[0])
    block_mix(ahead[0], 0)
    block_scores(ahead[1])
    block_mix(ahead[1], 1)
    for c in range(2):
        for i in range(parts):
            copy_out(c, i).wait()


def cache_and_decode(tp, table, reqs, pos, q, kn, vn, kp, vp, pre_pages, dec_pages, tile):
    n_q, _, rows, head = q.shape
    tokens = tp * rows
    pool, page, _ = kp.shape
    n_dec = table.shape[0] - 1
    parts = 4
    bf, f32 = jnp.bfloat16, jnp.float32
    full = jax.ShapeDtypeStruct(kp.shape, bf)
    line = jax.ShapeDtypeStruct((table.shape[1] * page, head), bf)
    early = jax.ShapeDtypeStruct((2, rows, n_q * head), bf)
    dma = pltpu.SemaphoreType.DMA
    return pl.pallas_call(
        functools.partial(cache_kernel, tp, tile, parts, head ** -0.5 * LOG2E, pre_pages, dec_pages),
        out_shape=[jax.ShapeDtypeStruct((n_dec, n_q * head), bf), full, full, line, line, early],
        in_specs=[SMEM] * 3 + [VMEM] * 3 + [ANY] * 2,
        out_specs=[VMEM, ANY, ANY, VMEM, VMEM, VMEM],
        scratch_shapes=[
            pltpu.VMEM(kp.shape, bf), pltpu.VMEM(kp.shape, bf),
            pltpu.VMEM((n_dec, 8, dec_pages * page), f32), pltpu.VMEM((n_dec, 8, head), f32),
            pltpu.VMEM((n_q, n_dec, head), f32), pltpu.VMEM((n_q, n_dec, head), f32),
            pltpu.VMEM((n_q, rows, line.shape[0]), f32), pltpu.VMEM((n_q, rows, head), f32),
            pltpu.VMEM((n_q, rows, head), f32), pltpu.VMEM((n_q, rows, head), f32),
            dma((2, parts)), dma((2, parts)),
        ],
        compiler_params=pltpu.CompilerParams(vmem_limit_bytes=67043328),
        cost_estimate=cost(4e10, 1e8),
        name="cache_and_decode",
    )(table, reqs, pos, q, kn, vn, kp, vp)


def attend_kernel(tp, parts, scale, tile, pre_len, q_any, dec, early, w_o_any, x_any, g, keys_any, vals_any, mid_out, hid_out,
                  w_o, x, q, keys, vals, in_sem, score, top, weight, acc, o,
                  psend, precv, ssend, rrecv, ps_sem, pr_sem, ss_sem, rr_sem):
    chips = tp // 2
    chip, core, peer, chip_at = ring_places(tp)
    nxt = 2 * chip_at(1) + core
    prv = 2 * chip_at(-1) + core
    n_q, _, rows, head = q.shape
    wide = psend.shape[3]
    span = keys.shape[0]
    pre_tiles, all_tiles = pre_len // tile, span // tile
    n_dec = dec.shape[0]
    loads = [pltpu.make_async_copy(a, b, in_sem.at[i]) for i, (a, b) in enumerate(
        ((w_o_any, w_o), (q_any, q), (keys_any, keys), (vals_any, vals), (x_any, x)))]
    for load in loads:
        load.start()
    greet(peer, nxt, prv)

    def to_peer(s, p):
        return remote(psend.at[lax.rem(s, 2), p], precv.at[s, p], ps_sem.at[s, p], pr_sem.at[s, p], peer)

    def to_next(s, p):
        return remote(ssend.at[s, p], rrecv.at[s, p], ss_sem.at[s, p], rr_sem.at[s, p], nxt)

    def theirs(s):
        return 2 * chip_at(s + 1) + 1 - core

    def mine(s):
        return 2 * chip_at(-(s + 1)) + core

    def tiles(block):
        return tile_count(block, rows, pre_len, span, tile)

    def scores(block, slot, t, masked):
        tile_scores(q, keys, score.at[slot], top.at[slot], block, t, tile, pre_len, masked)

    def mix(slot, t):
        tile_mix(vals, score.at[slot], top.at[slot], weight, acc, t, tile, scale)

    def finish(block):
        @pl.when(block == tp - 1)
        def _():
            o[pl.ds(rows - n_dec, n_dec), :] = dec[...]

    def run(slot, block, ahead, more):
        other = 1 - slot
        open_mix(top.at[slot], weight, acc)
        top[other] = jnp.full(top.shape[1:], -jnp.inf, jnp.float32)
        now = tiles(block)
        then = tiles(ahead) * more
        first = pre_len // tile * more

        def both(masked):
            def fn(t):
                scores(ahead, other, t, masked)
                mix(slot, t)
            return fn

        loop(0, first, both(False))
        joint = jnp.maximum(first, jnp.minimum(now, then))
        loop(first, joint, both(True))
        loop(joint, then, lambda t: scores(ahead, other, t, True))
        loop(joint, now, lambda t: mix(slot, t))
        close_mix(weight, acc, o)
        finish(block)

    def product(p):
        cols = pl.ds(pl.multiple_of(p * wide, wide), wide)
        return jnp.dot(o[...], w_o[:, cols], preferred_element_type=jnp.float32)

    def give_all(s):
        def give(p):
            @pl.when(s > 1)
            def _():
                to_peer(s - 2, p).wait_send()

            psend[lax.rem(s, 2), p] = product(p).astype(jnp.bfloat16)
            to_peer(s, p).start()

        loop(0, parts, give)

    def take_all(s):
        def take(p):
            own = product(p)
            to_peer(s, p).wait_recv()
            own = own + precv[s, p].astype(jnp.float32)
            cols = pl.ds(pl.multiple_of(p * wide, wide), wide)
            score[1, 0, :, cols] = own

            @pl.when(s > 0)
            def _():
                to_next(s - 1, p).wait_recv()
                score[1, 0, :, cols] = own + rrecv[s - 1, p].astype(jnp.float32)

            @pl.when(s < chips - 1)
            def _():
                ssend[s, p] = score[1, 0, :, cols].astype(jnp.bfloat16)
                to_next(s, p).start()

        loop(0, parts, take)

    def step(s, carry):
        @pl.when(s == 0)
        def _():
            o[...] = early[0]
            finish(theirs(0))

        @pl.when(s > 0)
        def _():
            run(0, theirs(s), mine(s), 1)

        give_all(s)

        @pl.when(s == 0)
        def _():
            o[...] = early[1]
            finish(mine(0))

        @pl.when(s > 0)
        def _():
            run(1, mine(s), theirs(s + 1), jnp.where(s < chips - 1, 1, 0))

        take_all(s)

        @pl.when(s == 0)
        def _():
            for load in loads[1:]:
                load.wait()
            top[0] = jnp.full(top.shape[1:], -jnp.inf, jnp.float32)
            loop(0, tiles(theirs(1)), lambda t: scores(theirs(1), 0, t, True))

        return carry

    loads[0].wait()
    lax.fori_loop(0, chips, step, 0)

    total = score.at[1, 0]
    square = jnp.zeros((rows, 1), jnp.float32)
    for p in range(parts):
        cols = slice(p * wide, (p + 1) * wide)
        mid = (x[:, cols].astype(jnp.float32) + total[:, cols].astype(jnp.bfloat16).astype(jnp.float32)).astype(jnp.bfloat16)
        mid_out[:, cols] = mid
        mid = mid.astype(jnp.float32)
        total[:, cols] = mid
        square = square + jnp.sum(mid * mid, axis=-1, keepdims=True)
    inv_rms = lax.rsqrt(square / (parts * wide) + EPS)
    for p in range(parts):
        cols = slice(p * wide, (p + 1) * wide)
        hid_out[:, cols] = (total[:, cols] * inv_rms * g[1:2, cols]).astype(jnp.bfloat16)
    for p in range(parts):
        for s in range(chips):
            if s >= chips - 2:
                to_peer(s, p).wait_send()
            if s < chips - 1:
                to_next(s, p).wait_send()


def attend_project(tp, q, dec, early, w_o, x, g, keys, vals, pre_len, tile):
    n_q, _, rows, head = q.shape
    d = x.shape[1]
    parts = 3
    wide = d // parts
    chips = tp // 2
    span = keys.shape[0]
    bf, f32 = jnp.bfloat16, jnp.float32
    dma = pltpu.SemaphoreType.DMA
    block = lambda n: pltpu.VMEM((n, parts, rows, wide), bf)
    out = jax.ShapeDtypeStruct((rows, d), bf)
    return pl.pallas_call(
        functools.partial(attend_kernel, tp, parts, head ** -0.5 * LOG2E, tile, pre_len),
        out_shape=[out, out],
        in_specs=[ANY, VMEM, VMEM, ANY, ANY, VMEM, ANY, ANY],
        out_specs=[VMEM] * 2,
        scratch_shapes=[
            pltpu.VMEM(w_o.shape, bf), pltpu.VMEM((rows, d), bf), pltpu.VMEM(q.shape, bf), pltpu.VMEM((span, head), bf), pltpu.VMEM((span, head), bf), dma((5,)),
            pltpu.VMEM((2, n_q, rows, span), f32), pltpu.VMEM((2, n_q, rows, head), f32),
            pltpu.VMEM((n_q, rows, head), f32), pltpu.VMEM((n_q, rows, head), f32),
            pltpu.VMEM((rows, n_q * head), bf),
            block(2), block(chips), block(chips - 1), block(chips - 1),
            dma((chips, parts)), dma((chips, parts)), dma((chips - 1, parts)), dma((chips - 1, parts)),
        ],
        compiler_params=pltpu.CompilerParams(collective_id=1, has_side_effects=True, vmem_limit_bytes=67043328),
        cost_estimate=cost(6e10, 1e7),
        name="attend_project",
    )(q, dec, early, w_o, x, g, keys, vals)


def mlp_kernel(tp, parts, hid, mid, w_gate, w_up, w_down, out,
               hbuf, gbuf, ubuf, dbuf, xbuf, act, acc, last, psend, precv, ssend, rrecv,
               in_sem, ag_s, ag_r, pg_s, pg_r, ps_sem, pr_sem, ss_sem, rr_sem):
    chips = tp // 2
    chip, core, peer, chip_at = ring_places(tp)
    nxt = 2 * chip_at(1) + core
    prv = 2 * chip_at(-1) + core
    _, rows, wide = acc.shape
    ff = gbuf.shape[1]
    tile = 256
    cut = 144
    halves = ((0, cut), (cut, rows - cut))
    loads = [pltpu.make_async_copy(a, b, in_sem.at[i]) for i, (a, b) in enumerate(
        ((hid, hbuf.at[0]), (w_gate, gbuf), (w_up, ubuf), (w_down, dbuf), (mid, xbuf)))]
    for load in loads:
        load.start()
    greet(peer, nxt, prv)

    def gather(j, i):
        first, n = halves[i]
        cut_rows = pl.ds(first, n)
        return remote(hbuf.at[j, cut_rows], hbuf.at[j + 1, cut_rows], ag_s.at[j, i], ag_r.at[j, i], nxt)

    def share(j):
        return remote(hbuf.at[j], hbuf.at[chips + j], pg_s.at[j], pg_r.at[j], peer)

    def to_peer(s, q):
        return remote(psend.at[s % 2, q], precv.at[s, q], ps_sem.at[s, q], pr_sem.at[s, q], peer)

    def to_next(s, q):
        return remote(ssend.at[s % 2, q], rrecv.at[s, q], ss_sem.at[s, q], rr_sem.at[s, q], nxt)

    def hidden_act(j):
        def body(t, carry):
            cols = pl.ds(pl.multiple_of(t * tile, tile), tile)
            gate = jnp.dot(hbuf[j], gbuf[:, cols], preferred_element_type=jnp.float32)
            up = jnp.dot(hbuf[j], ubuf[:, cols], preferred_element_type=jnp.float32)
            act[:, cols] = (gate * jax.nn.sigmoid(gate) * up).astype(jnp.bfloat16)
            return carry

        lax.fori_loop(0, ff // tile, body, 0)

    def down(q):
        cols = pl.ds(pl.multiple_of(q * wide, wide), wide)
        return jnp.dot(act[...], dbuf[:, cols], preferred_element_type=jnp.float32)

    def keep(j, dst):
        hidden_act(j)

        def body(q, carry):
            dst[q] = down(q)
            return carry

        lax.fori_loop(0, parts, body, 0)

    def give(j, s, before):
        hidden_act(j)

        def body(q, carry):
            if before is not None:
                to_peer(before, q).wait_send()
            psend[s % 2, q] = down(q).astype(jnp.bfloat16)
            to_peer(s, q).start()
            return carry

        lax.fori_loop(0, parts, body, 0)

    loads[0].wait()
    for i in range(2):
        gather(0, i).start()
    share(0).start()
    for load in loads[1:4]:
        load.wait()
    keep(0, last)
    share(0).wait_recv()
    end = chips - 1
    give(chips, end, None)
    for s in range(end):
        j = s + 1
        for i in range(2):
            gather(j - 1, i).wait_recv()
            if j < end:
                gather(j, i).start()
        share(j).start()
        keep(j, acc)
        share(j).wait_recv()
        give(chips + j, s, {0: None, 1: end, 2: 0}[s] if chips == 4 else None)

        def take(q, carry, s=s):
            to_peer(s, q).wait_recv()
            part = acc[q] + precv[s, q].astype(jnp.float32)
            if s > 0:
                to_next(s - 1, q).wait_recv()
                part = part + rrecv[s - 1, q].astype(jnp.float32)
            if s > 1:
                to_next(s - 2, q).wait_send()
            ssend[s % 2, q] = part.astype(jnp.bfloat16)
            to_next(s, q).start()
            return carry

        lax.fori_loop(0, parts, take, 0)

    loads[4].wait()
    for q in range(parts):
        cols = slice(q * wide, (q + 1) * wide)
        to_peer(end, q).wait_recv()
        part = last[q] + precv[end, q].astype(jnp.float32)
        to_next(end - 1, q).wait_recv()
        part = part + rrecv[end - 1, q].astype(jnp.float32)
        xbuf[:, cols] = (xbuf[:, cols].astype(jnp.float32) + part.astype(jnp.bfloat16).astype(jnp.float32)).astype(jnp.bfloat16)
    store = pltpu.make_async_copy(xbuf, out, in_sem.at[0])
    store.start()
    for j in range(chips):
        share(j).wait_send()
        if j < end:
            for i in range(2):
                gather(j, i).wait_send()
    for q in range(parts):
        to_peer(1, q).wait_send()
        to_peer(2, q).wait_send()
        for s in (end - 2, end - 1):
            to_next(s, q).wait_send()
    store.wait()


def mlp(tp, hid, mid, w_gate, w_up, w_down):
    rows, d = hid.shape
    ff = w_gate.shape[1]
    parts = 3
    wide = d // parts
    chips = tp // 2
    bf = jnp.bfloat16
    dma = pltpu.SemaphoreType.DMA
    block = lambda n: pltpu.VMEM((n, parts, rows, wide), bf)
    return pl.pallas_call(
        functools.partial(mlp_kernel, tp, parts),
        out_shape=jax.ShapeDtypeStruct((rows, d), bf),
        in_specs=[ANY] * 5,
        out_specs=ANY,
        scratch_shapes=[
            pltpu.VMEM((2 * chips, rows, d), bf),
            pltpu.VMEM((d, ff), bf), pltpu.VMEM((d, ff), bf), pltpu.VMEM((ff, d), bf),
            pltpu.VMEM((rows, d), bf), pltpu.VMEM((rows, ff), bf),
            pltpu.VMEM((parts, rows, wide), jnp.float32), pltpu.VMEM((parts, rows, wide), jnp.float32),
            block(2), block(chips), block(2), block(chips - 1),
            dma((5,)), dma((chips - 1, 2)), dma((chips - 1, 2)), dma((chips,)), dma((chips,)),
            dma((chips, parts)), dma((chips, parts)), dma((chips - 1, parts)), dma((chips - 1, parts)),
        ],
        compiler_params=pltpu.CompilerParams(collective_id=2, has_side_effects=True, vmem_limit_bytes=67043328),
        cost_estimate=cost(1e11, 2e7),
        name="mlp",
    )(hid, mid, w_gate, w_up, w_down)


def solution(mesh):
    tp = mesh.shape['tp']
    row_spec = P(('dp', 'tp'), None)
    group_vec = P('dp')
    table_spec = P('dp', None)
    cache_spec = P('dp', None, 'tp', None)
    col_split = P(None, 'tp')
    row_split = P('tp', None)
    gain_spec = P(None)

    def device_layer(x_in, req_ids, positions, block_table, ctx_len, k_pages, v_pages, w_q, w_k, w_v, w_o, w_gate, w_up, w_down, g_attn, g_mlp):
        pool, page, kv_heads, head = k_pages.shape
        tokens = positions.shape[0]
        n_dec = block_table.shape[0] - 1
        chunk_len = tokens - n_dec
        width = block_table.shape[1]
        pre_pages = width - chunk_len // page
        dec_pages = (pool - width) // n_dec
        n_q = w_q.shape[1] // head

        gains = jnp.stack([g_attn, g_mlp]).astype(jnp.float32)
        q, kn, vn = front(tp, positions, x_in, gains, w_q, w_k, w_v, head, n_dec, pre_pages * page)
        kn, vn = kn.reshape(tokens, head), vn.reshape(tokens, head)
        tile = 512
        dec, ko, vo, keys, vals, early = cache_and_decode(tp, block_table, req_ids, positions, q, kn, vn, k_pages.reshape(pool, page, head), v_pages.reshape(pool, page, head), pre_pages, dec_pages, tile)
        mid_rows, hidden_mlp = attend_project(tp, q, dec, early, w_o, x_in, gains, keys, vals, pre_pages * page, tile)
        x_out = mlp(tp, hidden_mlp, mid_rows, w_gate, w_up, w_down)
        return x_out, ko.reshape(k_pages.shape), vo.reshape(v_pages.shape)

    return jax.shard_map(device_layer, mesh=mesh, in_specs=(row_spec, group_vec, group_vec, table_spec, group_vec, cache_spec, cache_spec, col_split, col_split, col_split, row_split, col_split, col_split, row_split, gain_spec, gain_spec), out_specs=(row_spec, cache_spec, cache_spec), check_vma=False)
```

```python
import functools

import jax
import jax.numpy as jnp
import numpy as np
from jax import lax
from jax.experimental import pallas as pl
from jax.experimental.pallas import tpu as pltpu
from jax.sharding import PartitionSpec as P

EPS = 1e-5
THETA = 500000.0
LOG2E = 1.4426950408889634
ANY = pl.BlockSpec(memory_space=pl.ANY)
SMEM = pl.BlockSpec(memory_space=pltpu.SMEM)
VMEM = pl.BlockSpec(memory_space=pltpu.VMEM)


def cost(flops, nbytes):
    return pl.CostEstimate(flops=int(flops), bytes_accessed=int(nbytes), transcendentals=0)


def ring_places(tp):
    chips = tp // 2
    me = lax.axis_index('tp')
    chip, core = me // 2, lax.rem(me, 2)
    sign = 1 - 2 * core
    peer = 2 * chip + 1 - core

    def chip_at(offset):
        return lax.rem(chip + sign * offset + 2 * chips, chips)

    return chip, core, peer, chip_at


def greet(*others):
    barrier = pltpu.get_barrier_semaphore()
    for other in others:
        pl.semaphore_signal(barrier, inc=1, device_id={'tp': other}, device_id_type=pl.DeviceIdType.MESH)
    pl.semaphore_wait(barrier, len(others))


def remote(src, dst, send, recv, to):
    return pltpu.make_async_remote_copy(src_ref=src, dst_ref=dst, send_sem=send, recv_sem=recv, device_id={'tp': to}, device_id_type=pl.DeviceIdType.MESH)


def front_kernel(tp, start, n_dec, pos, x, g, freq, w_q, w_k, w_v, q_out, k_out, v_out,
                 hbuf, w, last_pos, w_sem, ag_s, ag_r, pg_s, pg_r):
    chips = tp // 2
    chip, core, peer, chip_at = ring_places(tp)
    nxt = 2 * chip_at(1) + core
    prv = 2 * chip_at(-1) + core
    rows, d = x.shape
    n_q = q_out.shape[0]
    head = k_out.shape[2]
    halves = ((0, 144), (144, rows - 144))

    def gather(j, i):
        at = pl.ds(*halves[i])
        return remote(hbuf.at[j, at], hbuf.at[j + 1, at], ag_s.at[j, i], ag_r.at[j, i], nxt)

    def share(j, i):
        at = pl.ds(*halves[i])
        return remote(hbuf.at[j, at], hbuf.at[chips + j, at], pg_s.at[j, i], pg_r.at[j, i], peer)

    w_cols = n_q * head
    loads = [
        pltpu.make_async_copy(w_q, w.at[:, pl.ds(0, w_cols)], w_sem.at[0]),
        pltpu.make_async_copy(w_k, w.at[:, pl.ds(w_cols, head)], w_sem.at[1]),
        pltpu.make_async_copy(w_v, w.at[:, pl.ds(w_cols + head, head)], w_sem.at[2]),
    ]
    for load in loads:
        load.start()
    rows32 = x[...].astype(jnp.float32)
    inv_rms = lax.rsqrt(jnp.mean(rows32 * rows32, axis=-1, keepdims=True) + EPS)
    hbuf[0] = (rows32 * inv_rms * g[0:1, :]).astype(jnp.bfloat16)
    greet(peer, nxt, prv)
    for i in range(2):
        gather(0, i).start()
    for i in range(2):
        share(0, i).start()

    def chunk_pos(block):
        return (lax.broadcasted_iota(jnp.int32, (rows, head), 0) + (start + block * rows)).astype(jnp.float32)

    last_pos[...] = chunk_pos(tp - 1)
    first = pos.shape[0] - n_dec

    def note(i, carry):
        last_pos[pl.ds(rows - n_dec + i, 1), :] = jnp.full((1, head), pos[first + i], jnp.int32).astype(jnp.float32)
        return carry

    lax.fori_loop(0, n_dec, note, 0, unroll=8)
    flip = jnp.where(lax.broadcasted_iota(jnp.int32, (1, head), 1) < head // 2, -1.0, 1.0)

    def qkv(j, block, i):
        lo, n = halves[i]
        at = pl.ds(lo, n)
        z = jnp.dot(hbuf[j, at, :], w[...], preferred_element_type=jnp.float32).astype(jnp.bfloat16)
        is_last = jnp.broadcast_to(block, (n, head)) == tp - 1
        angle = jnp.where(is_last, last_pos[at, :], chunk_pos(block)[lo:lo + n]) * freq[...]
        cs, sn = jnp.cos(angle), jnp.sin(angle) * flip
        for m in range(n_q + 1):
            part = z[:, m * head:(m + 1) * head].astype(jnp.float32)
            val = (part * cs + pltpu.roll(part, head // 2, 1) * sn).astype(jnp.bfloat16)
            if m < n_q:
                q_out[m, block, at, :] = val
            else:
                k_out[block, at, :] = val
        v_out[block, at, :] = z[:, (n_q + 1) * head:]

    for load in loads:
        load.wait()
    for i in range(2):
        qkv(0, 2 * chip + core, i)
    for i in range(2):
        share(0, i).wait_recv()
        qkv(chips, peer, i)

    def hop(j, carry):
        for i in range(2):
            gather(j - 1, i).wait_recv()

            @pl.when(j < chips - 1)
            def _():
                gather(j, i).start()

            share(j, i).start()
            qkv(j, 2 * chip_at(-j) + core, i)
            share(j, i).wait_recv()
            qkv(chips + j, 2 * chip_at(j) + 1 - core, i)
        return carry

    lax.fori_loop(1, chips, hop, 0)
    for j in range(chips):
        for i in range(2):
            share(j, i).wait_send()
            if j < chips - 1:
                gather(j, i).wait_send()


def front(tp, pos, x, g, w_q, w_k, w_v, head, n_dec, start):
    rows, d = x.shape
    n_q = w_q.shape[1] // head
    chips = tp // 2
    bf = jnp.bfloat16
    dma = pltpu.SemaphoreType.DMA
    shape = lambda *dims: jax.ShapeDtypeStruct(dims, bf)
    new = shape(tp, rows, head)
    freq = (THETA ** (-(np.arange(head) % (head // 2)) * 2.0 / head)).astype(np.float32)[None, :]
    return pl.pallas_call(
        functools.partial(front_kernel, tp, start, n_dec),
        out_shape=[shape(n_q, tp, rows, head), new, new],
        in_specs=[SMEM] + [VMEM] * 3 + [ANY] * 3,
        out_specs=[VMEM] * 3,
        scratch_shapes=[
            pltpu.VMEM((2 * chips, rows, d), bf),
            pltpu.VMEM((d, (n_q + 2) * head), bf),
            pltpu.VMEM((rows, head), jnp.float32),
            dma((3,)), dma((chips - 1, 2)), dma((chips - 1, 2)), dma((chips, 2)), dma((chips, 2)),
        ],
        compiler_params=pltpu.CompilerParams(collective_id=0, has_side_effects=True, vmem_limit_bytes=60 * 2**20),
        cost_estimate=cost(6e10, 1e7),
        name="front",
    )(pos, x, g, jnp.asarray(freq), w_q, w_k, w_v)


def lanes(fn, v, head):
    out = v[:, :head]
    for i in range(1, v.shape[1] // head):
        out = fn(out, v[:, i * head:(i + 1) * head])
    return out


def tile_at(t, tile):
    return pl.ds(pl.multiple_of(t * tile, tile), tile)


def tile_count(block, rows, pre_len, span, tile):
    return jnp.minimum(pre_len // tile + ((block + 1) * rows + tile - 1) // tile, span // tile)


def tile_scores(q, keys, score, top, block, t, tile, pre_len, masked):
    n_q, _, rows, head = q.shape
    kt = keys[tile_at(t, tile), :]
    if masked:
        diff = lax.broadcasted_iota(jnp.int32, (rows, tile), 1) - lax.broadcasted_iota(jnp.int32, (rows, tile), 0)
        seen = diff <= pre_len + block * rows - t * tile
    for n in range(n_q):
        s = lax.dot_general(q[n, block], kt, (((1,), (1,)), ((), ())), preferred_element_type=jnp.float32)
        if masked:
            s = jnp.where(seen, s, -1e30)
        score[n, :, tile_at(t, tile)] = s
        top[n] = jnp.maximum(top[n], lanes(jnp.maximum, s, head))


def tile_mix(vals, score, top, weight, acc, t, tile, scale):
    n_q, _, head = acc.shape
    vt = vals[tile_at(t, tile), :]
    for n in range(n_q):
        p = jnp.exp2((score[n, :, tile_at(t, tile)] - top[n, :, :1]) * scale)
        weight[n] += lanes(jnp.add, p, head)
        acc[n] += jnp.dot(p.astype(jnp.bfloat16), vt, preferred_element_type=jnp.float32)


def open_mix(top, weight, acc):
    for n in range(top.shape[0]):
        top[n] = jnp.broadcast_to(jnp.max(top[n], axis=-1, keepdims=True), top.shape[1:])
    weight[...] = jnp.zeros_like(weight)
    acc[...] = jnp.zeros_like(acc)


def close_mix(weight, acc, o):
    n_q, _, head = acc.shape
    for n in range(n_q):
        total = jnp.sum(weight[n], axis=-1, keepdims=True)
        o[:, n * head:(n + 1) * head] = (acc[n] / total).astype(jnp.bfloat16)


def loop(lo, hi, fn):
    def body(t, carry):
        fn(t)
        return carry

    lax.fori_loop(lo, hi, body, 0)


def cache_kernel(tp, tile, parts, scale, pre_pages, dec_pages, table, reqs, pos, q, kn, vn, kp, vp, out, ko, vo, kc, vc, early,
                 kbuf, vbuf, prob, total, qf, of, score_buf, top, weight, acc, in_sem, out_sem, pre_sem):
    n_q, n_dec, head = qf.shape
    rows = q.shape[2]
    chip, core, peer, chip_at = ring_places(tp)
    ahead = (2 * chip_at(1) + 1 - core, 2 * chip_at(-1) + core)
    pool, page, _ = kbuf.shape
    step = pool // parts
    chunk_len = reqs.shape[0] - n_dec
    chunk_pages = chunk_len // page
    some = 16
    wide = some * page
    pairs = ((kp, kbuf, ko, kn, kc), (vp, vbuf, vo, vn, vc))

    def copy_in(c, i):
        at = pl.ds(i * step, step)
        return pltpu.make_async_copy(pairs[c][0].at[at], pairs[c][1].at[at], in_sem.at[c, i])

    def copy_out(c, i):
        at = pl.ds(i * step, step)
        return pltpu.make_async_copy(pairs[c][1].at[at], pairs[c][2].at[at], out_sem.at[c, i])

    pre_len = pre_pages * page
    span = kc.shape[0]
    for c, (src, _, _, new, line) in enumerate(pairs):

        def fetch(i, carry, c=c, src=src, line=line):
            rows = pl.ds(pl.multiple_of(i * page, page), page)
            pltpu.make_async_copy(src.at[table[reqs[0], i]], line.at[rows, :], pre_sem.at[c]).start()
            return carry

        lax.fori_loop(0, pre_pages, fetch, 0, unroll=8)
    for c in range(2):
        for i in range(parts):
            copy_in(c, i).start()
    for c, (_, _, _, new, line) in enumerate(pairs):
        line[pl.ds(pre_len, chunk_len), :] = new[pl.ds(0, chunk_len), :]
    qf[...] = q[:, tp - 1, pl.ds(rows - n_dec, n_dec), :].astype(jnp.float32)
    req0 = reqs[0]

    def arrive(c):
        _, buf, _, new, _ = pairs[c]
        for i in range(parts):
            copy_in(c, i).wait()

        def chunk(i, carry):
            buf[table[req0, pre_pages + i]] = new[pl.ds(pl.multiple_of(i * page, page), page), :]
            return carry

        lax.fori_loop(0, chunk_pages, chunk, 0, unroll=8)
        fresh = new[pl.ds(chunk_len, n_dec), :].astype(jnp.float32)
        of[c] = fresh

        def decode(i, carry):
            p = pos[chunk_len + i]
            at = table[reqs[chunk_len + i], p // page]
            hit = lax.broadcasted_iota(jnp.int32, (page, head), 0) == lax.rem(p, page)
            row = jnp.broadcast_to(of[c, pl.ds(i, 1), :], (page, head))
            buf[at] = jnp.where(hit, row, buf[at].astype(jnp.float32)).astype(jnp.bfloat16)
            return carry

        lax.fori_loop(0, n_dec, decode, 0, unroll=4)
        for i in range(parts):
            copy_out(c, i).start()

    def some_pages(buf, req, t):
        return jnp.concatenate([buf[table[req, t * some + j]] for j in range(some)], axis=0)

    col = lax.broadcasted_iota(jnp.int32, (8, dec_pages * page), 1)
    blank = jnp.zeros((8 - n_q, head), jnp.float32)
    both = 8

    def block_scores(block):
        top[...] = jnp.full(top.shape, -jnp.inf, jnp.float32)
        loop(0, tile_count(block, rows, pre_len, span, tile),
             lambda t: tile_scores(q, kc, score_buf, top, block, t, tile, pre_len, True))

    def block_mix(block, e):
        open_mix(top, weight, acc)
        loop(0, tile_count(block, rows, pre_len, span, tile),
             lambda t: tile_mix(vc, score_buf, top, weight, acc, t, tile, scale))
        close_mix(weight, acc, early.at[e])

    for c, line in enumerate((kc, vc)):
        whole = line.at[pl.ds(0, pre_len), :]
        pltpu.make_async_copy(whole, whole, pre_sem.at[c]).wait()
    for e in range(2):
        block_scores(ahead[e])
        block_mix(ahead[e], e)
    arrive(0)
    arrive(1)

    def score(g, carry):
        for r in range(both):
            i = g * both + r
            req = reqs[chunk_len + i]
            qr = jnp.concatenate([qf[n, pl.ds(i, 1), :] for n in range(n_q)] + [blank], axis=0).astype(jnp.bfloat16)
            s = jnp.concatenate([
                lax.dot_general(qr, some_pages(kbuf, req, t), (((1,), (1,)), ((), ())), preferred_element_type=jnp.float32)
                for t in range(dec_pages // some)], axis=1)
            s = jnp.where(col <= pos[chunk_len + i], s, -1e30)
            p = jnp.exp2((s - jnp.max(s, axis=-1, keepdims=True)) * scale)
            total[i] = jnp.broadcast_to(jnp.sum(p, axis=-1, keepdims=True), (8, head))
            prob[i] = p
        return carry

    lax.fori_loop(0, n_dec // both, score, 0)

    def mix(g, carry):
        for r in range(both):
            i = g * both + r
            req = reqs[chunk_len + i]
            o = sum(
                jnp.dot(prob[i, :, t * wide:(t + 1) * wide].astype(jnp.bfloat16), some_pages(vbuf, req, t), preferred_element_type=jnp.float32)
                for t in range(dec_pages // some))
            o = o / total[i]
            for n in range(n_q):
                of[n, pl.ds(i, 1), :] = o[n:n + 1]
        return carry

    lax.fori_loop(0, n_dec // both, mix, 0)
    for n in range(n_q):
        out[:, n * head:(n + 1) * head] = of[n].astype(jnp.bfloat16)
    for c in range(2):
        for i in range(parts):
            copy_out(c, i).wait()


def cache_and_decode(tp, table, reqs, pos, q, kn, vn, kp, vp, pre_pages, dec_pages, tile):
    n_q, _, rows, head = q.shape
    tokens = tp * rows
    pool, page, _ = kp.shape
    n_dec = table.shape[0] - 1
    parts = 4
    bf, f32 = jnp.bfloat16, jnp.float32
    full = jax.ShapeDtypeStruct(kp.shape, bf)
    line = jax.ShapeDtypeStruct((table.shape[1] * page, head), bf)
    early = jax.ShapeDtypeStruct((2, rows, n_q * head), bf)
    dma = pltpu.SemaphoreType.DMA
    return pl.pallas_call(
        functools.partial(cache_kernel, tp, tile, parts, head ** -0.5 * LOG2E, pre_pages, dec_pages),
        out_shape=[jax.ShapeDtypeStruct((n_dec, n_q * head), bf), full, full, line, line, early],
        in_specs=[SMEM] * 3 + [VMEM] * 3 + [ANY] * 2,
        out_specs=[VMEM, ANY, ANY, VMEM, VMEM, VMEM],
        scratch_shapes=[
            pltpu.VMEM(kp.shape, bf), pltpu.VMEM(kp.shape, bf),
            pltpu.VMEM((n_dec, 8, dec_pages * page), f32), pltpu.VMEM((n_dec, 8, head), f32),
            pltpu.VMEM((n_q, n_dec, head), f32), pltpu.VMEM((n_q, n_dec, head), f32),
            pltpu.VMEM((n_q, rows, line.shape[0]), f32), pltpu.VMEM((n_q, rows, head), f32),
            pltpu.VMEM((n_q, rows, head), f32), pltpu.VMEM((n_q, rows, head), f32),
            dma((2, parts)), dma((2, parts)), dma((2,)),
        ],
        compiler_params=pltpu.CompilerParams(vmem_limit_bytes=67043328),
        cost_estimate=cost(4e10, 1e8),
        name="cache_and_decode",
    )(table, reqs, pos, q, kn, vn, kp, vp)


def attend_kernel(tp, parts, scale, tile, pre_len, q_any, dec, early, w_o_any, x_any, g, keys_any, vals_any, mid_out, hid_out,
                  w_o, x, q, keys, vals, in_sem, score, top, weight, acc, o,
                  psend, precv, ssend, rrecv, ps_sem, pr_sem, ss_sem, rr_sem):
    chips = tp // 2
    chip, core, peer, chip_at = ring_places(tp)
    nxt = 2 * chip_at(1) + core
    prv = 2 * chip_at(-1) + core
    n_q, _, rows, head = q.shape
    wide = psend.shape[3]
    span = keys.shape[0]
    pre_tiles, all_tiles = pre_len // tile, span // tile
    n_dec = dec.shape[0]
    loads = [pltpu.make_async_copy(a, b, in_sem.at[i]) for i, (a, b) in enumerate(
        ((w_o_any, w_o), (q_any, q), (keys_any, keys), (vals_any, vals), (x_any, x)))]
    for load in loads:
        load.start()
    greet(peer, nxt, prv)

    def to_peer(s, p):
        return remote(psend.at[lax.rem(s, 2), p], precv.at[s, p], ps_sem.at[s, p], pr_sem.at[s, p], peer)

    def to_next(s, p):
        return remote(ssend.at[s, p], rrecv.at[s, p], ss_sem.at[s, p], rr_sem.at[s, p], nxt)

    def theirs(s):
        return 2 * chip_at(s + 1) + 1 - core

    def mine(s):
        return 2 * chip_at(-(s + 1)) + core

    def tiles(block):
        return tile_count(block, rows, pre_len, span, tile)

    def scores(block, slot, t, masked):
        tile_scores(q, keys, score.at[slot], top.at[slot], block, t, tile, pre_len, masked)

    def mix(slot, t):
        tile_mix(vals, score.at[slot], top.at[slot], weight, acc, t, tile, scale)

    def finish(block):
        @pl.when(block == tp - 1)
        def _():
            o[pl.ds(rows - n_dec, n_dec), :] = dec[...]

    def run(slot, block, ahead, more):
        other = 1 - slot
        open_mix(top.at[slot], weight, acc)
        top[other] = jnp.full(top.shape[1:], -jnp.inf, jnp.float32)
        now = tiles(block)
        then = tiles(ahead) * more
        first = pre_len // tile * more

        def both(masked):
            def fn(t):
                scores(ahead, other, t, masked)
                mix(slot, t)
            return fn

        loop(0, first, both(False))
        joint = jnp.maximum(first, jnp.minimum(now, then))
        loop(first, joint, both(True))
        loop(joint, then, lambda t: scores(ahead, other, t, True))
        loop(joint, now, lambda t: mix(slot, t))
        close_mix(weight, acc, o)
        finish(block)

    def product(p):
        cols = pl.ds(pl.multiple_of(p * wide, wide), wide)
        return jnp.dot(o[...], w_o[:, cols], preferred_element_type=jnp.float32)

    def give_all(s):
        def give(p):
            @pl.when(s > 1)
            def _():
                to_peer(s - 2, p).wait_send()

            psend[lax.rem(s, 2), p] = product(p).astype(jnp.bfloat16)
            to_peer(s, p).start()

        loop(0, parts, give)

    def take_all(s):
        def take(p):
            own = product(p)
            to_peer(s, p).wait_recv()
            own = own + precv[s, p].astype(jnp.float32)
            cols = pl.ds(pl.multiple_of(p * wide, wide), wide)
            score[1, 0, :, cols] = own

            @pl.when(s > 0)
            def _():
                to_next(s - 1, p).wait_recv()
                score[1, 0, :, cols] = own + rrecv[s - 1, p].astype(jnp.float32)

            @pl.when(s < chips - 1)
            def _():
                ssend[s, p] = score[1, 0, :, cols].astype(jnp.bfloat16)
                to_next(s, p).start()

        loop(0, parts, take)

    def step(s, carry):
        @pl.when(s == 0)
        def _():
            o[...] = early[0]
            finish(theirs(0))

        @pl.when(s > 0)
        def _():
            run(0, theirs(s), mine(s), 1)

        give_all(s)

        @pl.when(s == 0)
        def _():
            o[...] = early[1]
            finish(mine(0))

        @pl.when(s > 0)
        def _():
            run(1, mine(s), theirs(s + 1), jnp.where(s < chips - 1, 1, 0))

        take_all(s)

        @pl.when(s == 0)
        def _():
            for load in loads[1:]:
                load.wait()
            top[0] = jnp.full(top.shape[1:], -jnp.inf, jnp.float32)
            loop(0, tiles(theirs(1)), lambda t: scores(theirs(1), 0, t, True))

        return carry

    loads[0].wait()
    lax.fori_loop(0, chips, step, 0)

    total = score.at[1, 0]
    square = jnp.zeros((rows, 1), jnp.float32)
    for p in range(parts):
        cols = slice(p * wide, (p + 1) * wide)
        mid = (x[:, cols].astype(jnp.float32) + total[:, cols].astype(jnp.bfloat16).astype(jnp.float32)).astype(jnp.bfloat16)
        mid_out[:, cols] = mid
        mid = mid.astype(jnp.float32)
        total[:, cols] = mid
        square = square + jnp.sum(mid * mid, axis=-1, keepdims=True)
    inv_rms = lax.rsqrt(square / (parts * wide) + EPS)
    for p in range(parts):
        cols = slice(p * wide, (p + 1) * wide)
        hid_out[:, cols] = (total[:, cols] * inv_rms * g[1:2, cols]).astype(jnp.bfloat16)
    for p in range(parts):
        for s in range(chips):
            if s >= chips - 2:
                to_peer(s, p).wait_send()
            if s < chips - 1:
                to_next(s, p).wait_send()


def attend_project(tp, q, dec, early, w_o, x, g, keys, vals, pre_len, tile):
    n_q, _, rows, head = q.shape
    d = x.shape[1]
    parts = 3
    wide = d // parts
    chips = tp // 2
    span = keys.shape[0]
    bf, f32 = jnp.bfloat16, jnp.float32
    dma = pltpu.SemaphoreType.DMA
    block = lambda n: pltpu.VMEM((n, parts, rows, wide), bf)
    out = jax.ShapeDtypeStruct((rows, d), bf)
    return pl.pallas_call(
        functools.partial(attend_kernel, tp, parts, head ** -0.5 * LOG2E, tile, pre_len),
        out_shape=[out, out],
        in_specs=[ANY, VMEM, VMEM, ANY, ANY, VMEM, ANY, ANY],
        out_specs=[VMEM] * 2,
        scratch_shapes=[
            pltpu.VMEM(w_o.shape, bf), pltpu.VMEM((rows, d), bf), pltpu.VMEM(q.shape, bf), pltpu.VMEM((span, head), bf), pltpu.VMEM((span, head), bf), dma((5,)),
            pltpu.VMEM((2, n_q, rows, span), f32), pltpu.VMEM((2, n_q, rows, head), f32),
            pltpu.VMEM((n_q, rows, head), f32), pltpu.VMEM((n_q, rows, head), f32),
            pltpu.VMEM((rows, n_q * head), bf),
            block(2), block(chips), block(chips - 1), block(chips - 1),
            dma((chips, parts)), dma((chips, parts)), dma((chips - 1, parts)), dma((chips - 1, parts)),
        ],
        compiler_params=pltpu.CompilerParams(collective_id=1, has_side_effects=True, vmem_limit_bytes=67043328),
        cost_estimate=cost(6e10, 1e7),
        name="attend_project",
    )(q, dec, early, w_o, x, g, keys, vals)


def mlp_kernel(tp, parts, hid, mid, w_gate, w_up, w_down, out,
               hbuf, gbuf, ubuf, dbuf, xbuf, act, acc, last, psend, precv, ssend, rrecv,
               in_sem, ag_s, ag_r, pg_s, pg_r, ps_sem, pr_sem, ss_sem, rr_sem):
    chips = tp // 2
    chip, core, peer, chip_at = ring_places(tp)
    nxt = 2 * chip_at(1) + core
    prv = 2 * chip_at(-1) + core
    _, rows, wide = acc.shape
    ff = gbuf.shape[1]
    tile = 256
    cut = 144
    halves = ((0, cut), (cut, rows - cut))
    loads = [pltpu.make_async_copy(a, b, in_sem.at[i]) for i, (a, b) in enumerate(
        ((hid, hbuf.at[0]), (w_gate, gbuf), (w_up, ubuf), (w_down, dbuf), (mid, xbuf)))]
    for load in loads:
        load.start()
    greet(peer, nxt, prv)

    def gather(j, i):
        first, n = halves[i]
        cut_rows = pl.ds(first, n)
        return remote(hbuf.at[j, cut_rows], hbuf.at[j + 1, cut_rows], ag_s.at[j, i], ag_r.at[j, i], nxt)

    def share(j):
        return remote(hbuf.at[j], hbuf.at[chips + j], pg_s.at[j], pg_r.at[j], peer)

    def to_peer(s, q):
        return remote(psend.at[s % 2, q], precv.at[s, q], ps_sem.at[s, q], pr_sem.at[s, q], peer)

    def to_next(s, q):
        return remote(ssend.at[s % 2, q], rrecv.at[s, q], ss_sem.at[s, q], rr_sem.at[s, q], nxt)

    def hidden_act(j):
        def body(t, carry):
            cols = pl.ds(pl.multiple_of(t * tile, tile), tile)
            gate = jnp.dot(hbuf[j], gbuf[:, cols], preferred_element_type=jnp.float32)
            up = jnp.dot(hbuf[j], ubuf[:, cols], preferred_element_type=jnp.float32)
            act[:, cols] = (gate * jax.nn.sigmoid(gate) * up).astype(jnp.bfloat16)
            return carry

        lax.fori_loop(0, ff // tile, body, 0)

    def down(q):
        cols = pl.ds(pl.multiple_of(q * wide, wide), wide)
        return jnp.dot(act[...], dbuf[:, cols], preferred_element_type=jnp.float32)

    def keep(j, dst):
        hidden_act(j)

        def body(q, carry):
            dst[q] = down(q)
            return carry

        lax.fori_loop(0, parts, body, 0)

    def give(j, s, before):
        hidden_act(j)

        def body(q, carry):
            if before is not None:
                to_peer(before, q).wait_send()
            psend[s % 2, q] = down(q).astype(jnp.bfloat16)
            to_peer(s, q).start()
            return carry

        lax.fori_loop(0, parts, body, 0)

    loads[0].wait()
    for i in range(2):
        gather(0, i).start()
    share(0).start()
    for load in loads[1:4]:
        load.wait()
    keep(0, last)
    share(0).wait_recv()
    end = chips - 1
    give(chips, end, None)
    for s in range(end):
        j = s + 1
        for i in range(2):
            gather(j - 1, i).wait_recv()
            if j < end:
                gather(j, i).start()
        share(j).start()
        keep(j, acc)
        share(j).wait_recv()
        give(chips + j, s, {0: None, 1: end, 2: 0}[s] if chips == 4 else None)

        def take(q, carry, s=s):
            to_peer(s, q).wait_recv()
            part = acc[q] + precv[s, q].astype(jnp.float32)
            if s > 0:
                to_next(s - 1, q).wait_recv()
                part = part + rrecv[s - 1, q].astype(jnp.float32)
            if s > 1:
                to_next(s - 2, q).wait_send()
            ssend[s % 2, q] = part.astype(jnp.bfloat16)
            to_next(s, q).start()
            return carry

        lax.fori_loop(0, parts, take, 0)

    loads[4].wait()
    for q in range(parts):
        cols = slice(q * wide, (q + 1) * wide)
        to_peer(end, q).wait_recv()
        part = last[q] + precv[end, q].astype(jnp.float32)
        to_next(end - 1, q).wait_recv()
        part = part + rrecv[end - 1, q].astype(jnp.float32)
        xbuf[:, cols] = (xbuf[:, cols].astype(jnp.float32) + part.astype(jnp.bfloat16).astype(jnp.float32)).astype(jnp.bfloat16)
    store = pltpu.make_async_copy(xbuf, out, in_sem.at[0])
    store.start()
    for j in range(chips):
        share(j).wait_send()
        if j < end:
            for i in range(2):
                gather(j, i).wait_send()
    for q in range(parts):
        to_peer(1, q).wait_send()
        to_peer(2, q).wait_send()
        for s in (end - 2, end - 1):
            to_next(s, q).wait_send()
    store.wait()


def mlp(tp, hid, mid, w_gate, w_up, w_down):
    rows, d = hid.shape
    ff = w_gate.shape[1]
    parts = 3
    wide = d // parts
    chips = tp // 2
    bf = jnp.bfloat16
    dma = pltpu.SemaphoreType.DMA
    block = lambda n: pltpu.VMEM((n, parts, rows, wide), bf)
    return pl.pallas_call(
        functools.partial(mlp_kernel, tp, parts),
        out_shape=jax.ShapeDtypeStruct((rows, d), bf),
        in_specs=[ANY] * 5,
        out_specs=ANY,
        scratch_shapes=[
            pltpu.VMEM((2 * chips, rows, d), bf),
            pltpu.VMEM((d, ff), bf), pltpu.VMEM((d, ff), bf), pltpu.VMEM((ff, d), bf),
            pltpu.VMEM((rows, d), bf), pltpu.VMEM((rows, ff), bf),
            pltpu.VMEM((parts, rows, wide), jnp.float32), pltpu.VMEM((parts, rows, wide), jnp.float32),
            block(2), block(chips), block(2), block(chips - 1),
            dma((5,)), dma((chips - 1, 2)), dma((chips - 1, 2)), dma((chips,)), dma((chips,)),
            dma((chips, parts)), dma((chips, parts)), dma((chips - 1, parts)), dma((chips - 1, parts)),
        ],
        compiler_params=pltpu.CompilerParams(collective_id=2, has_side_effects=True, vmem_limit_bytes=67043328),
        cost_estimate=cost(1e11, 2e7),
        name="mlp",
    )(hid, mid, w_gate, w_up, w_down)


def solution(mesh):
    tp = mesh.shape['tp']
    row_spec = P(('dp', 'tp'), None)
    group_vec = P('dp')
    table_spec = P('dp', None)
    cache_spec = P('dp', None, 'tp', None)
    col_split = P(None, 'tp')
    row_split = P('tp', None)
    gain_spec = P(None)

    def device_layer(x_in, req_ids, positions, block_table, ctx_len, k_pages, v_pages, w_q, w_k, w_v, w_o, w_gate, w_up, w_down, g_attn, g_mlp):
        pool, page, kv_heads, head = k_pages.shape
        tokens = positions.shape[0]
        n_dec = block_table.shape[0] - 1
        chunk_len = tokens - n_dec
        width = block_table.shape[1]
        pre_pages = width - chunk_len // page
        dec_pages = (pool - width) // n_dec
        n_q = w_q.shape[1] // head

        gains = jnp.stack([g_attn, g_mlp]).astype(jnp.float32)
        q, kn, vn = front(tp, positions, x_in, gains, w_q, w_k, w_v, head, n_dec, pre_pages * page)
        kn, vn = kn.reshape(tokens, head), vn.reshape(tokens, head)
        tile = 512
        dec, ko, vo, keys, vals, early = cache_and_decode(tp, block_table, req_ids, positions, q, kn, vn, k_pages.reshape(pool, page, head), v_pages.reshape(pool, page, head), pre_pages, dec_pages, tile)
        mid_rows, hidden_mlp = attend_project(tp, q, dec, early, w_o, x_in, gains, keys, vals, pre_pages * page, tile)
        x_out = mlp(tp, hidden_mlp, mid_rows, w_gate, w_up, w_down)
        return x_out, ko.reshape(k_pages.shape), vo.reshape(v_pages.shape)

    return jax.shard_map(device_layer, mesh=mesh, in_specs=(row_spec, group_vec, group_vec, table_spec, group_vec, cache_spec, cache_spec, col_split, col_split, col_split, row_split, col_split, col_split, row_split, gain_spec, gain_spec), out_specs=(row_spec, cache_spec, cache_spec), check_vma=False)
```

```python
import functools

import jax
import jax.numpy as jnp
import numpy as np
from jax import lax
from jax.experimental import pallas as pl
from jax.experimental.pallas import tpu as pltpu
from jax.sharding import PartitionSpec as P

EPS = 1e-5
THETA = 500000.0
LOG2E = 1.4426950408889634
ANY = pl.BlockSpec(memory_space=pl.ANY)
SMEM = pl.BlockSpec(memory_space=pltpu.SMEM)
VMEM = pl.BlockSpec(memory_space=pltpu.VMEM)


def cost(flops, nbytes):
    return pl.CostEstimate(flops=int(flops), bytes_accessed=int(nbytes), transcendentals=0)


def ring_places(tp):
    chips = tp // 2
    me = lax.axis_index('tp')
    chip, core = me // 2, lax.rem(me, 2)
    sign = 1 - 2 * core
    peer = 2 * chip + 1 - core

    def chip_at(offset):
        return lax.rem(chip + sign * offset + 2 * chips, chips)

    return chip, core, peer, chip_at


def greet(*others):
    barrier = pltpu.get_barrier_semaphore()
    for other in others:
        pl.semaphore_signal(barrier, inc=1, device_id={'tp': other}, device_id_type=pl.DeviceIdType.MESH)
    pl.semaphore_wait(barrier, len(others))


def remote(src, dst, send, recv, to):
    return pltpu.make_async_remote_copy(src_ref=src, dst_ref=dst, send_sem=send, recv_sem=recv, device_id={'tp': to}, device_id_type=pl.DeviceIdType.MESH)


def front_kernel(tp, start, n_dec, pos, x, g, freq, w_q, w_k, w_v, q_out, k_out, v_out,
                 hbuf, w, last_pos, w_sem, ag_s, ag_r, pg_s, pg_r):
    chips = tp // 2
    chip, core, peer, chip_at = ring_places(tp)
    nxt = 2 * chip_at(1) + core
    prv = 2 * chip_at(-1) + core
    rows, d = x.shape
    n_q = q_out.shape[0]
    head = k_out.shape[2]
    halves = ((0, 144), (144, rows - 144))

    def gather(j, i):
        at = pl.ds(*halves[i])
        return remote(hbuf.at[j, at], hbuf.at[j + 1, at], ag_s.at[j, i], ag_r.at[j, i], nxt)

    def share(j, i):
        at = pl.ds(*halves[i])
        return remote(hbuf.at[j, at], hbuf.at[chips + j, at], pg_s.at[j, i], pg_r.at[j, i], peer)

    w_cols = n_q * head
    loads = [
        pltpu.make_async_copy(w_q, w.at[:, pl.ds(0, w_cols)], w_sem.at[0]),
        pltpu.make_async_copy(w_k, w.at[:, pl.ds(w_cols, head)], w_sem.at[1]),
        pltpu.make_async_copy(w_v, w.at[:, pl.ds(w_cols + head, head)], w_sem.at[2]),
    ]
    for load in loads:
        load.start()
    rows32 = x[...].astype(jnp.float32)
    inv_rms = lax.rsqrt(jnp.mean(rows32 * rows32, axis=-1, keepdims=True) + EPS)
    hbuf[0] = (rows32 * inv_rms * g[0:1, :]).astype(jnp.bfloat16)
    greet(peer, nxt, prv)
    for i in range(2):
        gather(0, i).start()
    for i in range(2):
        share(0, i).start()

    def chunk_pos(block):
        return (lax.broadcasted_iota(jnp.int32, (rows, head), 0) + (start + block * rows)).astype(jnp.float32)

    last_pos[...] = chunk_pos(tp - 1)
    first = pos.shape[0] - n_dec

    def note(i, carry):
        last_pos[pl.ds(rows - n_dec + i, 1), :] = jnp.full((1, head), pos[first + i], jnp.int32).astype(jnp.float32)
        return carry

    lax.fori_loop(0, n_dec, note, 0, unroll=8)
    flip = jnp.where(lax.broadcasted_iota(jnp.int32, (1, head), 1) < head // 2, -1.0, 1.0)

    def qkv(j, block, i):
        lo, n = halves[i]
        at = pl.ds(lo, n)
        z = jnp.dot(hbuf[j, at, :], w[...], preferred_element_type=jnp.float32).astype(jnp.bfloat16)
        is_last = jnp.broadcast_to(block, (n, head)) == tp - 1
        angle = jnp.where(is_last, last_pos[at, :], chunk_pos(block)[lo:lo + n]) * freq[...]
        cs, sn = jnp.cos(angle), jnp.sin(angle) * flip
        for m in range(n_q + 1):
            part = z[:, m * head:(m + 1) * head].astype(jnp.float32)
            val = (part * cs + pltpu.roll(part, head // 2, 1) * sn).astype(jnp.bfloat16)
            if m < n_q:
                q_out[m, block, at, :] = val
            else:
                k_out[block, at, :] = val
        v_out[block, at, :] = z[:, (n_q + 1) * head:]

    for load in loads:
        load.wait()
    for i in range(2):
        qkv(0, 2 * chip + core, i)
    for i in range(2):
        share(0, i).wait_recv()
        qkv(chips, peer, i)

    def hop(j, carry):
        for i in range(2):
            gather(j - 1, i).wait_recv()

            @pl.when(j < chips - 1)
            def _():
                gather(j, i).start()

            share(j, i).start()
            qkv(j, 2 * chip_at(-j) + core, i)
            share(j, i).wait_recv()
            qkv(chips + j, 2 * chip_at(j) + 1 - core, i)
        return carry

    lax.fori_loop(1, chips, hop, 0)
    for j in range(chips):
        for i in range(2):
            share(j, i).wait_send()
            if j < chips - 1:
                gather(j, i).wait_send()


def front(tp, pos, x, g, w_q, w_k, w_v, head, n_dec, start):
    rows, d = x.shape
    n_q = w_q.shape[1] // head
    chips = tp // 2
    bf = jnp.bfloat16
    dma = pltpu.SemaphoreType.DMA
    shape = lambda *dims: jax.ShapeDtypeStruct(dims, bf)
    new = shape(tp, rows, head)
    freq = (THETA ** (-(np.arange(head) % (head // 2)) * 2.0 / head)).astype(np.float32)[None, :]
    return pl.pallas_call(
        functools.partial(front_kernel, tp, start, n_dec),
        out_shape=[shape(n_q, tp, rows, head), new, new],
        in_specs=[SMEM] + [VMEM] * 3 + [ANY] * 3,
        out_specs=[VMEM] * 3,
        scratch_shapes=[
            pltpu.VMEM((2 * chips, rows, d), bf),
            pltpu.VMEM((d, (n_q + 2) * head), bf),
            pltpu.VMEM((rows, head), jnp.float32),
            dma((3,)), dma((chips - 1, 2)), dma((chips - 1, 2)), dma((chips, 2)), dma((chips, 2)),
        ],
        compiler_params=pltpu.CompilerParams(collective_id=0, has_side_effects=True, vmem_limit_bytes=60 * 2**20),
        cost_estimate=cost(6e10, 1e7),
        name="front",
    )(pos, x, g, jnp.asarray(freq), w_q, w_k, w_v)


def lanes(fn, v, head):
    out = v[:, :head]
    for i in range(1, v.shape[1] // head):
        out = fn(out, v[:, i * head:(i + 1) * head])
    return out


def tile_at(t, tile):
    return pl.ds(pl.multiple_of(t * tile, tile), tile)


def tile_count(block, rows, pre_len, span, tile):
    return jnp.minimum(pre_len // tile + ((block + 1) * rows + tile - 1) // tile, span // tile)


def tile_scores(q, keys, score, top, block, t, tile, pre_len, masked):
    n_q, _, rows, head = q.shape
    kt = keys[tile_at(t, tile), :]
    if masked:
        diff = lax.broadcasted_iota(jnp.int32, (rows, tile), 1) - lax.broadcasted_iota(jnp.int32, (rows, tile), 0)
        seen = diff <= pre_len + block * rows - t * tile
    for n in range(n_q):
        s = lax.dot_general(q[n, block], kt, (((1,), (1,)), ((), ())), preferred_element_type=jnp.float32)
        if masked:
            s = jnp.where(seen, s, -1e30)
        score[n, :, tile_at(t, tile)] = s
        top[n] = jnp.maximum(top[n], lanes(jnp.maximum, s, head))


def tile_mix(vals, score, top, weight, acc, t, tile, scale):
    n_q, _, head = acc.shape
    vt = vals[tile_at(t, tile), :]
    for n in range(n_q):
        p = jnp.exp2((score[n, :, tile_at(t, tile)] - top[n, :, :1]) * scale)
        weight[n] += lanes(jnp.add, p, head)
        acc[n] += jnp.dot(p.astype(jnp.bfloat16), vt, preferred_element_type=jnp.float32)


def open_mix(top, weight, acc):
    for n in range(top.shape[0]):
        top[n] = jnp.broadcast_to(jnp.max(top[n], axis=-1, keepdims=True), top.shape[1:])
    weight[...] = jnp.zeros_like(weight)
    acc[...] = jnp.zeros_like(acc)


def close_mix(weight, acc, o):
    n_q, _, head = acc.shape
    for n in range(n_q):
        total = jnp.sum(weight[n], axis=-1, keepdims=True)
        o[:, n * head:(n + 1) * head] = (acc[n] / total).astype(jnp.bfloat16)


def loop(lo, hi, fn):
    def body(t, carry):
        fn(t)
        return carry

    lax.fori_loop(lo, hi, body, 0)


def cache_kernel(tp, tile, parts, scale, pre_pages, dec_pages, table, reqs, pos, q, kn, vn, kp, vp, out, ko, vo, kc, vc, early,
                 kbuf, vbuf, qf, of, score_buf, top, weight, acc, in_sem, out_sem, pre_sem):
    n_q, n_dec, head = qf.shape
    rows = q.shape[2]
    chip, core, peer, chip_at = ring_places(tp)
    ahead = (2 * chip_at(1) + 1 - core, 2 * chip_at(-1) + core)
    pool, page, _ = kbuf.shape
    step = pool // parts
    chunk_len = reqs.shape[0] - n_dec
    chunk_pages = chunk_len // page
    some = 16
    wide = some * page
    pairs = ((kp, kbuf, ko, kn, kc), (vp, vbuf, vo, vn, vc))

    def copy_in(c, i):
        at = pl.ds(i * step, step)
        return pltpu.make_async_copy(pairs[c][0].at[at], pairs[c][1].at[at], in_sem.at[c, i])

    def copy_out(c, i):
        at = pl.ds(i * step, step)
        return pltpu.make_async_copy(pairs[c][1].at[at], pairs[c][2].at[at], out_sem.at[c, i])

    pre_len = pre_pages * page
    span = kc.shape[0]
    for c, (src, _, _, new, line) in enumerate(pairs):

        def fetch(i, carry, c=c, src=src, line=line):
            rows = pl.ds(pl.multiple_of(i * page, page), page)
            pltpu.make_async_copy(src.at[table[reqs[0], i]], line.at[rows, :], pre_sem.at[c]).start()
            return carry

        lax.fori_loop(0, pre_pages, fetch, 0, unroll=8)
    for c in range(2):
        for i in range(parts):
            copy_in(c, i).start()
    for c, (_, _, _, new, line) in enumerate(pairs):
        line[pl.ds(pre_len, chunk_len), :] = new[pl.ds(0, chunk_len), :]
    qf[...] = q[:, tp - 1, pl.ds(rows - n_dec, n_dec), :].astype(jnp.float32)
    req0 = reqs[0]

    def arrive(c):
        _, buf, _, new, _ = pairs[c]
        for i in range(parts):
            copy_in(c, i).wait()

        def chunk(i, carry):
            buf[table[req0, pre_pages + i]] = new[pl.ds(pl.multiple_of(i * page, page), page), :]
            return carry

        lax.fori_loop(0, chunk_pages, chunk, 0, unroll=8)
        fresh = new[pl.ds(chunk_len, n_dec), :].astype(jnp.float32)
        of[c] = fresh

        def decode(i, carry):
            p = pos[chunk_len + i]
            at = table[reqs[chunk_len + i], p // page]
            hit = lax.broadcasted_iota(jnp.int32, (page, head), 0) == lax.rem(p, page)
            row = jnp.broadcast_to(of[c, pl.ds(i, 1), :], (page, head))
            buf[at] = jnp.where(hit, row, buf[at].astype(jnp.float32)).astype(jnp.bfloat16)
            return carry

        lax.fori_loop(0, n_dec, decode, 0, unroll=4)
        for i in range(parts):
            copy_out(c, i).start()

    def some_pages(buf, req, t):
        return jnp.concatenate([buf[table[req, t * some + j]] for j in range(some)], axis=0)

    col = lax.broadcasted_iota(jnp.int32, (8, dec_pages * page), 1)
    blank = jnp.zeros((8 - n_q, head), jnp.float32)
    both = 8

    def block_scores(block):
        top[...] = jnp.full(top.shape, -jnp.inf, jnp.float32)
        loop(0, tile_count(block, rows, pre_len, span, tile),
             lambda t: tile_scores(q, kc, score_buf, top, block, t, tile, pre_len, True))

    def block_mix(block, e):
        open_mix(top, weight, acc)
        loop(0, tile_count(block, rows, pre_len, span, tile),
             lambda t: tile_mix(vc, score_buf, top, weight, acc, t, tile, scale))
        close_mix(weight, acc, early.at[e])

    for c, line in enumerate((kc, vc)):
        whole = line.at[pl.ds(0, pre_len), :]
        pltpu.make_async_copy(whole, whole, pre_sem.at[c]).wait()
    for e in range(2):
        block_scores(ahead[e])
        block_mix(ahead[e], e)
    arrive(0)
    arrive(1)

    def score(g, carry):
        for r in range(both):
            i = g * both + r
            req = reqs[chunk_len + i]
            qr = jnp.concatenate([qf[n, pl.ds(i, 1), :] for n in range(n_q)] + [blank], axis=0).astype(jnp.bfloat16)
            s = jnp.concatenate([
                lax.dot_general(qr, some_pages(kbuf, req, t), (((1,), (1,)), ((), ())), preferred_element_type=jnp.float32)
                for t in range(dec_pages // some)], axis=1)
            s = jnp.where(col <= pos[chunk_len + i], s, -1e30)
            p = jnp.exp2((s - jnp.max(s, axis=-1, keepdims=True)) * scale)
            o = sum(
                jnp.dot(p[:, t * wide:(t + 1) * wide].astype(jnp.bfloat16), some_pages(vbuf, req, t), preferred_element_type=jnp.float32)
                for t in range(dec_pages // some))
            o = o / jnp.sum(p, axis=-1, keepdims=True)
            for n in range(n_q):
                of[n, pl.ds(i, 1), :] = o[n:n + 1]
        return carry

    lax.fori_loop(0, n_dec // both, score, 0)
    for n in range(n_q):
        out[:, n * head:(n + 1) * head] = of[n].astype(jnp.bfloat16)
    for c in range(2):
        for i in range(parts):
            copy_out(c, i).wait()


def cache_and_decode(tp, table, reqs, pos, q, kn, vn, kp, vp, pre_pages, dec_pages, tile):
    n_q, _, rows, head = q.shape
    tokens = tp * rows
    pool, page, _ = kp.shape
    n_dec = table.shape[0] - 1
    parts = 4
    bf, f32 = jnp.bfloat16, jnp.float32
    full = jax.ShapeDtypeStruct(kp.shape, bf)
    line = jax.ShapeDtypeStruct((table.shape[1] * page, head), bf)
    early = jax.ShapeDtypeStruct((2, rows, n_q * head), bf)
    dma = pltpu.SemaphoreType.DMA
    return pl.pallas_call(
        functools.partial(cache_kernel, tp, tile, parts, head ** -0.5 * LOG2E, pre_pages, dec_pages),
        out_shape=[jax.ShapeDtypeStruct((n_dec, n_q * head), bf), full, full, line, line, early],
        in_specs=[SMEM] * 3 + [VMEM] * 3 + [ANY] * 2,
        out_specs=[VMEM, ANY, ANY, VMEM, VMEM, VMEM],
        scratch_shapes=[
            pltpu.VMEM(kp.shape, bf), pltpu.VMEM(kp.shape, bf),
            pltpu.VMEM((n_q, n_dec, head), f32), pltpu.VMEM((n_q, n_dec, head), f32),
            pltpu.VMEM((n_q, rows, line.shape[0]), f32), pltpu.VMEM((n_q, rows, head), f32),
            pltpu.VMEM((n_q, rows, head), f32), pltpu.VMEM((n_q, rows, head), f32),
            dma((2, parts)), dma((2, parts)), dma((2,)),
        ],
        compiler_params=pltpu.CompilerParams(vmem_limit_bytes=67043328),
        cost_estimate=cost(4e10, 1e8),
        name="cache_and_decode",
    )(table, reqs, pos, q, kn, vn, kp, vp)


def attend_kernel(tp, parts, scale, tile, pre_len, q_any, dec, early, w_o_any, x_any, g, keys_any, vals_any, mid_out, hid_out,
                  w_o, x, q, keys, vals, in_sem, score, top, weight, acc, o,
                  psend, precv, ssend, rrecv, ps_sem, pr_sem, ss_sem, rr_sem):
    chips = tp // 2
    chip, core, peer, chip_at = ring_places(tp)
    nxt = 2 * chip_at(1) + core
    prv = 2 * chip_at(-1) + core
    n_q, _, rows, head = q.shape
    wide = psend.shape[3]
    span = keys.shape[0]
    pre_tiles, all_tiles = pre_len // tile, span // tile
    n_dec = dec.shape[0]
    loads = [pltpu.make_async_copy(a, b, in_sem.at[i]) for i, (a, b) in enumerate(
        ((w_o_any, w_o), (q_any, q), (keys_any, keys), (vals_any, vals), (x_any, x)))]
    for load in loads:
        load.start()
    greet(peer, nxt, prv)

    def to_peer(s, p):
        return remote(psend.at[lax.rem(s, 2), p], precv.at[s, p], ps_sem.at[s, p], pr_sem.at[s, p], peer)

    def to_next(s, p):
        return remote(ssend.at[s, p], rrecv.at[s, p], ss_sem.at[s, p], rr_sem.at[s, p], nxt)

    def theirs(s):
        return 2 * chip_at(s + 1) + 1 - core

    def mine(s):
        return 2 * chip_at(-(s + 1)) + core

    def tiles(block):
        return tile_count(block, rows, pre_len, span, tile)

    def scores(block, slot, t, masked):
        tile_scores(q, keys, score.at[slot], top.at[slot], block, t, tile, pre_len, masked)

    def mix(slot, t):
        tile_mix(vals, score.at[slot], top.at[slot], weight, acc, t, tile, scale)

    def finish(block):
        @pl.when(block == tp - 1)
        def _():
            o[pl.ds(rows - n_dec, n_dec), :] = dec[...]

    def run(slot, block, ahead, more):
        other = 1 - slot
        open_mix(top.at[slot], weight, acc)
        top[other] = jnp.full(top.shape[1:], -jnp.inf, jnp.float32)
        now = tiles(block)
        then = tiles(ahead) * more
        first = pre_len // tile * more

        def both(masked):
            def fn(t):
                scores(ahead, other, t, masked)
                mix(slot, t)
            return fn

        loop(0, first, both(False))
        joint = jnp.maximum(first, jnp.minimum(now, then))
        loop(first, joint, both(True))
        loop(joint, then, lambda t: scores(ahead, other, t, True))
        loop(joint, now, lambda t: mix(slot, t))
        close_mix(weight, acc, o)
        finish(block)

    def product(p):
        cols = pl.ds(pl.multiple_of(p * wide, wide), wide)
        return jnp.dot(o[...], w_o[:, cols], preferred_element_type=jnp.float32)

    def give_all(s):
        def give(p):
            @pl.when(s > 1)
            def _():
                to_peer(s - 2, p).wait_send()

            psend[lax.rem(s, 2), p] = product(p).astype(jnp.bfloat16)
            to_peer(s, p).start()

        loop(0, parts, give)

    def take_all(s):
        def take(p):
            own = product(p)
            to_peer(s, p).wait_recv()
            own = own + precv[s, p].astype(jnp.float32)
            cols = pl.ds(pl.multiple_of(p * wide, wide), wide)
            score[1, 0, :, cols] = own

            @pl.when(s > 0)
            def _():
                to_next(s - 1, p).wait_recv()
                score[1, 0, :, cols] = own + rrecv[s - 1, p].astype(jnp.float32)

            @pl.when(s < chips - 1)
            def _():
                ssend[s, p] = score[1, 0, :, cols].astype(jnp.bfloat16)
                to_next(s, p).start()

        loop(0, parts, take)

    def step(s, carry):
        @pl.when(s == 0)
        def _():
            o[...] = early[0]
            finish(theirs(0))

        @pl.when(s > 0)
        def _():
            run(0, theirs(s), mine(s), 1)

        give_all(s)

        @pl.when(s == 0)
        def _():
            o[...] = early[1]
            finish(mine(0))

        @pl.when(s > 0)
        def _():
            run(1, mine(s), theirs(s + 1), jnp.where(s < chips - 1, 1, 0))

        take_all(s)

        @pl.when(s == 0)
        def _():
            for load in loads[1:]:
                load.wait()
            top[0] = jnp.full(top.shape[1:], -jnp.inf, jnp.float32)
            loop(0, tiles(theirs(1)), lambda t: scores(theirs(1), 0, t, True))

        return carry

    loads[0].wait()
    lax.fori_loop(0, chips, step, 0)

    total = score.at[1, 0]
    square = jnp.zeros((rows, 1), jnp.float32)
    for p in range(parts):
        cols = slice(p * wide, (p + 1) * wide)
        mid = (x[:, cols].astype(jnp.float32) + total[:, cols].astype(jnp.bfloat16).astype(jnp.float32)).astype(jnp.bfloat16)
        mid_out[:, cols] = mid
        mid = mid.astype(jnp.float32)
        total[:, cols] = mid
        square = square + jnp.sum(mid * mid, axis=-1, keepdims=True)
    inv_rms = lax.rsqrt(square / (parts * wide) + EPS)
    for p in range(parts):
        cols = slice(p * wide, (p + 1) * wide)
        hid_out[:, cols] = (total[:, cols] * inv_rms * g[1:2, cols]).astype(jnp.bfloat16)
    for p in range(parts):
        for s in range(chips):
            if s >= chips - 2:
                to_peer(s, p).wait_send()
            if s < chips - 1:
                to_next(s, p).wait_send()


def attend_project(tp, q, dec, early, w_o, x, g, keys, vals, pre_len, tile):
    n_q, _, rows, head = q.shape
    d = x.shape[1]
    parts = 3
    wide = d // parts
    chips = tp // 2
    span = keys.shape[0]
    bf, f32 = jnp.bfloat16, jnp.float32
    dma = pltpu.SemaphoreType.DMA
    block = lambda n: pltpu.VMEM((n, parts, rows, wide), bf)
    out = jax.ShapeDtypeStruct((rows, d), bf)
    return pl.pallas_call(
        functools.partial(attend_kernel, tp, parts, head ** -0.5 * LOG2E, tile, pre_len),
        out_shape=[out, out],
        in_specs=[ANY, VMEM, VMEM, ANY, ANY, VMEM, ANY, ANY],
        out_specs=[VMEM] * 2,
        scratch_shapes=[
            pltpu.VMEM(w_o.shape, bf), pltpu.VMEM((rows, d), bf), pltpu.VMEM(q.shape, bf), pltpu.VMEM((span, head), bf), pltpu.VMEM((span, head), bf), dma((5,)),
            pltpu.VMEM((2, n_q, rows, span), f32), pltpu.VMEM((2, n_q, rows, head), f32),
            pltpu.VMEM((n_q, rows, head), f32), pltpu.VMEM((n_q, rows, head), f32),
            pltpu.VMEM((rows, n_q * head), bf),
            block(2), block(chips), block(chips - 1), block(chips - 1),
            dma((chips, parts)), dma((chips, parts)), dma((chips - 1, parts)), dma((chips - 1, parts)),
        ],
        compiler_params=pltpu.CompilerParams(collective_id=1, has_side_effects=True, vmem_limit_bytes=67043328),
        cost_estimate=cost(6e10, 1e7),
        name="attend_project",
    )(q, dec, early, w_o, x, g, keys, vals)


def mlp_kernel(tp, parts, hid, mid, w_gate, w_up, w_down, out,
               hbuf, gbuf, ubuf, dbuf, xbuf, act, acc, last, psend, precv, ssend, rrecv,
               in_sem, ag_s, ag_r, pg_s, pg_r, ps_sem, pr_sem, ss_sem, rr_sem):
    chips = tp // 2
    chip, core, peer, chip_at = ring_places(tp)
    nxt = 2 * chip_at(1) + core
    prv = 2 * chip_at(-1) + core
    _, rows, wide = acc.shape
    ff = gbuf.shape[1]
    tile = 256
    cut = 144
    halves = ((0, cut), (cut, rows - cut))
    loads = [pltpu.make_async_copy(a, b, in_sem.at[i]) for i, (a, b) in enumerate(
        ((hid, hbuf.at[0]), (w_gate, gbuf), (w_up, ubuf), (w_down, dbuf), (mid, xbuf)))]
    for load in loads:
        load.start()
    greet(peer, nxt, prv)

    def gather(j, i):
        first, n = halves[i]
        cut_rows = pl.ds(first, n)
        return remote(hbuf.at[j, cut_rows], hbuf.at[j + 1, cut_rows], ag_s.at[j, i], ag_r.at[j, i], nxt)

    def share(j):
        return remote(hbuf.at[j], hbuf.at[chips + j], pg_s.at[j], pg_r.at[j], peer)

    def to_peer(s, q):
        return remote(psend.at[s % 2, q], precv.at[s, q], ps_sem.at[s, q], pr_sem.at[s, q], peer)

    def to_next(s, q):
        return remote(ssend.at[s % 2, q], rrecv.at[s, q], ss_sem.at[s, q], rr_sem.at[s, q], nxt)

    def hidden_act(j):
        def body(t, carry):
            cols = pl.ds(pl.multiple_of(t * tile, tile), tile)
            gate = jnp.dot(hbuf[j], gbuf[:, cols], preferred_element_type=jnp.float32)
            up = jnp.dot(hbuf[j], ubuf[:, cols], preferred_element_type=jnp.float32)
            act[:, cols] = (gate * jax.nn.sigmoid(gate) * up).astype(jnp.bfloat16)
            return carry

        lax.fori_loop(0, ff // tile, body, 0)

    def down(q):
        cols = pl.ds(pl.multiple_of(q * wide, wide), wide)
        return jnp.dot(act[...], dbuf[:, cols], preferred_element_type=jnp.float32)

    def keep(j, dst):
        hidden_act(j)

        def body(q, carry):
            dst[q] = down(q)
            return carry

        lax.fori_loop(0, parts, body, 0)

    def give(j, s, before):
        hidden_act(j)

        def body(q, carry):
            if before is not None:
                to_peer(before, q).wait_send()
            psend[s % 2, q] = down(q).astype(jnp.bfloat16)
            to_peer(s, q).start()
            return carry

        lax.fori_loop(0, parts, body, 0)

    loads[0].wait()
    for i in range(2):
        gather(0, i).start()
    share(0).start()
    for load in loads[1:4]:
        load.wait()
    keep(0, last)
    share(0).wait_recv()
    end = chips - 1
    give(chips, end, None)
    for s in range(end):
        j = s + 1
        for i in range(2):
            gather(j - 1, i).wait_recv()
            if j < end:
                gather(j, i).start()
        share(j).start()
        keep(j, acc)
        share(j).wait_recv()
        give(chips + j, s, {0: None, 1: end, 2: 0}[s] if chips == 4 else None)

        def take(q, carry, s=s):
            to_peer(s, q).wait_recv()
            part = acc[q] + precv[s, q].astype(jnp.float32)
            if s > 0:
                to_next(s - 1, q).wait_recv()
                part = part + rrecv[s - 1, q].astype(jnp.float32)
            if s > 1:
                to_next(s - 2, q).wait_send()
            ssend[s % 2, q] = part.astype(jnp.bfloat16)
            to_next(s, q).start()
            return carry

        lax.fori_loop(0, parts, take, 0)

    loads[4].wait()
    for q in range(parts):
        cols = slice(q * wide, (q + 1) * wide)
        to_peer(end, q).wait_recv()
        part = last[q] + precv[end, q].astype(jnp.float32)
        to_next(end - 1, q).wait_recv()
        part = part + rrecv[end - 1, q].astype(jnp.float32)
        xbuf[:, cols] = (xbuf[:, cols].astype(jnp.float32) + part.astype(jnp.bfloat16).astype(jnp.float32)).astype(jnp.bfloat16)
    store = pltpu.make_async_copy(xbuf, out, in_sem.at[0])
    store.start()
    for j in range(chips):
        share(j).wait_send()
        if j < end:
            for i in range(2):
                gather(j, i).wait_send()
    for q in range(parts):
        to_peer(1, q).wait_send()
        to_peer(2, q).wait_send()
        for s in (end - 2, end - 1):
            to_next(s, q).wait_send()
    store.wait()


def mlp(tp, hid, mid, w_gate, w_up, w_down):
    rows, d = hid.shape
    ff = w_gate.shape[1]
    parts = 3
    wide = d // parts
    chips = tp // 2
    bf = jnp.bfloat16
    dma = pltpu.SemaphoreType.DMA
    block = lambda n: pltpu.VMEM((n, parts, rows, wide), bf)
    return pl.pallas_call(
        functools.partial(mlp_kernel, tp, parts),
        out_shape=jax.ShapeDtypeStruct((rows, d), bf),
        in_specs=[ANY] * 5,
        out_specs=ANY,
        scratch_shapes=[
            pltpu.VMEM((2 * chips, rows, d), bf),
            pltpu.VMEM((d, ff), bf), pltpu.VMEM((d, ff), bf), pltpu.VMEM((ff, d), bf),
            pltpu.VMEM((rows, d), bf), pltpu.VMEM((rows, ff), bf),
            pltpu.VMEM((parts, rows, wide), jnp.float32), pltpu.VMEM((parts, rows, wide), jnp.float32),
            block(2), block(chips), block(2), block(chips - 1),
            dma((5,)), dma((chips - 1, 2)), dma((chips - 1, 2)), dma((chips,)), dma((chips,)),
            dma((chips, parts)), dma((chips, parts)), dma((chips - 1, parts)), dma((chips - 1, parts)),
        ],
        compiler_params=pltpu.CompilerParams(collective_id=2, has_side_effects=True, vmem_limit_bytes=67043328),
        cost_estimate=cost(1e11, 2e7),
        name="mlp",
    )(hid, mid, w_gate, w_up, w_down)


def solution(mesh):
    tp = mesh.shape['tp']
    row_spec = P(('dp', 'tp'), None)
    group_vec = P('dp')
    table_spec = P('dp', None)
    cache_spec = P('dp', None, 'tp', None)
    col_split = P(None, 'tp')
    row_split = P('tp', None)
    gain_spec = P(None)

    def device_layer(x_in, req_ids, positions, block_table, ctx_len, k_pages, v_pages, w_q, w_k, w_v, w_o, w_gate, w_up, w_down, g_attn, g_mlp):
        pool, page, kv_heads, head = k_pages.shape
        tokens = positions.shape[0]
        n_dec = block_table.shape[0] - 1
        chunk_len = tokens - n_dec
        width = block_table.shape[1]
        pre_pages = width - chunk_len // page
        dec_pages = (pool - width) // n_dec
        n_q = w_q.shape[1] // head

        gains = jnp.stack([g_attn, g_mlp]).astype(jnp.float32)
        q, kn, vn = front(tp, positions, x_in, gains, w_q, w_k, w_v, head, n_dec, pre_pages * page)
        kn, vn = kn.reshape(tokens, head), vn.reshape(tokens, head)
        tile = 512
        dec, ko, vo, keys, vals, early = cache_and_decode(tp, block_table, req_ids, positions, q, kn, vn, k_pages.reshape(pool, page, head), v_pages.reshape(pool, page, head), pre_pages, dec_pages, tile)
        mid_rows, hidden_mlp = attend_project(tp, q, dec, early, w_o, x_in, gains, keys, vals, pre_pages * page, tile)
        x_out = mlp(tp, hidden_mlp, mid_rows, w_gate, w_up, w_down)
        return x_out, ko.reshape(k_pages.shape), vo.reshape(v_pages.shape)

    return jax.shard_map(device_layer, mesh=mesh, in_specs=(row_spec, group_vec, group_vec, table_spec, group_vec, cache_spec, cache_spec, col_split, col_split, col_split, row_split, col_split, col_split, row_split, gain_spec, gain_spec), out_specs=(row_spec, cache_spec, cache_spec), check_vma=False)
```
